128 devices in a mesh: blk: 32 (over z, y, x_hi), tp: 4 (over x_lo, core).
Axes of the slice: x: 4 (x_hi: 2, x_lo: 2; x = x_hi * 2 + x_lo), y: 4, z: 4, core: 2. Of those that a mesh axis runs over, the one named last changes fastest.
Arguments:
- tokens: bfloat16 [8192, 2048], P('blk'), may hold values from -27 to 27
- order: int32 [64], replicated, may hold values from 0 to 63, each once
- gain_attn: float32 [2048], replicated, may hold values from 0.1 to 1.9
- gain_ffn: float32 [2048], replicated, may hold values from 0.1 to 1.9
- w_query: bfloat16 [2048, 2048], P(None, 'tp'), may hold values from -3.7565048 to 3.7565048
- w_key: bfloat16 [2048, 512], P(None, 'tp'), may hold values from -0.13258252 to 0.13258252
- w_value: bfloat16 [2048, 512], P(None, 'tp'), may hold values from -0.125 to 0.125
- w_out: bfloat16 [2048, 2048], P('tp'), may hold values from -0.125 to 0.125
- w_gate: bfloat16 [2048, 8192], P(None, 'tp'), may hold values from -0.125 to 0.125
- w_up: bfloat16 [2048, 8192], P(None, 'tp'), may hold values from -0.125 to 0.125
- w_down: bfloat16 [8192, 2048], P('tp'), may hold values from -0.0625 to 0.0625
Outputs:
- layer_out: bfloat16 [8192, 2048], P('blk', 'tp')
The draws below stay inside these ranges and needn't reach their ends.
Inputs may be any that keep to these rules, and one draw needn't show every extreme that they name: `order`: every number 0 to 63 appears once; device b of blk holds stored blocks 2b and 2b + 1.
All inputs are finite; a program needn't handle non-finite values.
Results may differ from the reference program's by a relative error of at most 0.0095.
Values may be sent and summed in bfloat16 or wider, within the bound.
A program may use at most 128 MiB of HBM per device.

```python
import math
import jax
import jax.numpy as jnp
from jax import lax

D = 2048
QH = 32
KVH = 8
HD = 64
FF = 8192
TOK_DEV = 256
SEQ = 8192
NCHUNK = 64
N_TP = 4


def shared_key_weight(key):
    base = jax.random.normal(jax.random.fold_in(key, 11), (D, KVH * HD), jnp.float32)
    return jnp.clip(base, -6.0, 6.0) * D ** (-0.5)


def draw_w_key(key, part):
    return shared_key_weight(key).astype(jnp.bfloat16)


def draw_w_query(key, part):
    noise = jax.random.normal(jax.random.fold_in(key, 12), (D, QH * HD), jnp.float32)
    noise = jnp.clip(noise, -6.0, 6.0) * (3.0 * D ** (-0.5))
    return noise.astype(jnp.bfloat16)


def draw_tokens(key, part):
    column = jnp.arange(D, dtype=jnp.float32) / (D - 1.0)
    rough = jax.random.uniform(jax.random.fold_in(key, 21), (D,), jnp.float32, 0.7, 1.3)
    col_scale = 0.5 * 4.0 ** column * rough
    base = jnp.clip(jax.random.normal(jax.random.fold_in(key, 24), (SEQ, D), jnp.float32), -6.0, 6.0)
    result = base * col_scale[None, :]
    return result.astype(jnp.bfloat16)


def level_of(rng, extent, shards, smallest, largest):
    factor_of = 1.0
    for dim, shards_of in shards:
        draws = jax.random.uniform(jax.random.fold_in(jax.random.fold_in(rng, 6), dim), (shards_of,), jnp.float32, smallest / len(shards), largest / len(shards))
        factor_of = factor_of * jnp.repeat(jnp.exp(draws), extent[dim] // shards_of).reshape((-1,) + (1,) * (len(extent) - 1 - dim))
    return factor_of


def normal_values(stream_key, shape, deviation, most, pieces=(), held_as=jnp.bfloat16):
    values = jax.random.normal(stream_key, shape, jnp.float32) * deviation
    if len(pieces) > 0:
        values = level_of(stream_key, shape, pieces, -0.22, 0.18) * values
    return jnp.clip(values, min=-most, max=most).astype(held_as)


def setup_inputs(seed: int = 0) -> dict:
    streams_of = jax.random.split(jax.random.key(seed), 12)
    return {
        "tokens": draw_tokens(jax.random.fold_in(streams_of[11], 71), 0),
        "order": jax.random.permutation(streams_of[1], NCHUNK).astype(jnp.int32),
        "gain_attn": jnp.clip(1.0 + 0.18 * jax.random.normal(streams_of[2], (D,), jnp.float32), 0.1, 1.9),
        "gain_ffn": jnp.clip(1.0 + 0.18 * jax.random.normal(streams_of[3], (D,), jnp.float32), 0.1, 1.9),
        "w_query": draw_w_query(jax.random.fold_in(streams_of[11], 71), 0),
        "w_key": draw_w_key(jax.random.fold_in(streams_of[11], 71), 0),
        "w_value": normal_values(streams_of[6], (D, KVH * HD), D ** -0.5, 0.125, ((1, 4),)),
        "w_out": normal_values(streams_of[7], (QH * HD, D), (QH * HD) ** -0.5, 0.125, ((0, 4),)),
        "w_gate": normal_values(streams_of[8], (D, FF), D ** -0.5, 0.125, ((1, 4),)),
        "w_up": normal_values(streams_of[9], (D, FF), D ** -0.5, 0.125, ((1, 4),)),
        "w_down": normal_values(streams_of[10], (FF, D), FF ** -0.5, 0.0625, ((0, 4),)),
    }


EPS = 1e-05
ROPE_BASE = 500000.0
MASKED = -1e+30

def rotate(values, positions):
    half_dim = values.shape[-1] // 2
    freq = ROPE_BASE ** (-(jnp.arange(half_dim, dtype=jnp.float32) * 2.0 / values.shape[-1]))
    angle = positions.astype(jnp.float32)[:, None] * freq[None, :]
    cosine = jnp.cos(angle)[:, None, :]
    sine = jnp.sin(angle)[:, None, :]
    first = values[..., :half_dim]
    second = values[..., half_dim:]
    return jnp.concatenate([first * cosine - second * sine, second * cosine + first * sine], axis=-1)

def reference(tokens, order, gain_attn, gain_ffn, w_query, w_key, w_value, w_out, w_gate, w_up, w_down):
    seq_len = tokens.shape[0]
    half_rows = TOK_DEV // 2
    stored = jnp.arange(seq_len, dtype=jnp.int32)
    position = order[stored // half_rows].astype(jnp.int32) * half_rows + stored % half_rows
    tokens_wide = tokens.astype(jnp.float32)
    normed = (tokens_wide * lax.rsqrt(lax.optimization_barrier(jnp.mean(tokens_wide * tokens_wide, axis=-1, keepdims=True)) + EPS) * gain_attn).astype(jnp.bfloat16)
    queries = jnp.dot(normed, w_query, preferred_element_type=jnp.float32).reshape(seq_len, QH, HD)
    queries = rotate(queries, position).astype(jnp.bfloat16)
    keys = jnp.dot(normed, w_key, preferred_element_type=jnp.float32).reshape(seq_len, KVH, HD)
    keys = rotate(keys, position).astype(jnp.bfloat16)
    values = jnp.dot(normed, w_value, preferred_element_type=jnp.float32).astype(jnp.bfloat16).reshape(seq_len, KVH, HD)
    group = QH // KVH
    query_block = math.gcd(seq_len, 256)
    grouped = queries.reshape(seq_len // query_block, query_block, KVH, group, HD)
    key_wide = keys.astype(jnp.float32)
    value_wide = values.astype(jnp.float32)
    scale = HD ** (-0.5)

    def one_block(inputs):
        block_queries, block_pos = inputs
        scores = jnp.einsum('qkgd,skd->kgqs', block_queries.astype(jnp.float32), key_wide) * scale
        allowed = position[None, :] <= block_pos[:, None]
        scores = jnp.where(allowed, scores, MASKED)
        highest = lax.optimization_barrier(jnp.max(scores, axis=-1, keepdims=True))
        weights = jnp.where(allowed, jnp.exp(scores - highest), 0.0)
        denominator = lax.optimization_barrier(jnp.sum(weights, axis=-1))
        rounded = lax.optimization_barrier(weights.astype(jnp.bfloat16)).astype(jnp.float32)
        mixed = jnp.einsum('kgqs,skd->qkgd', rounded, value_wide)
        return (mixed / jnp.transpose(denominator, (2, 0, 1))[..., None]).astype(jnp.bfloat16)
    heads = lax.map(one_block, (grouped, position.reshape(-1, query_block)))
    heads = heads.reshape(seq_len, QH * HD)
    head_share = QH * HD // N_TP
    attention = jnp.zeros((seq_len, D), jnp.float32)
    for member in range(N_TP):
        lower = member * head_share
        partial_value = jnp.dot(heads[:, lower:lower + head_share], w_out[lower:lower + head_share], preferred_element_type=jnp.float32)
        attention = attention + lax.optimization_barrier(partial_value.astype(jnp.bfloat16)).astype(jnp.float32)
    residual = tokens_wide + attention
    normed_ffn = (residual * lax.rsqrt(lax.optimization_barrier(jnp.mean(residual * residual, axis=-1, keepdims=True)) + EPS) * gain_ffn).astype(jnp.bfloat16)
    gate = jnp.dot(normed_ffn, w_gate, preferred_element_type=jnp.float32)
    up_proj = jnp.dot(normed_ffn, w_up, preferred_element_type=jnp.float32)
    hidden = (jax.nn.silu(gate) * up_proj).astype(jnp.bfloat16)
    unit_share = FF // N_TP
    feed = jnp.zeros((seq_len, D), jnp.float32)
    for member in range(N_TP):
        lower = member * unit_share
        partial_value = jnp.dot(hidden[:, lower:lower + unit_share], w_down[lower:lower + unit_share], preferred_element_type=jnp.float32)
        feed = feed + lax.optimization_barrier(partial_value.astype(jnp.bfloat16)).astype(jnp.float32)
    return (residual + feed).astype(jnp.bfloat16)
```

```python
import functools

import jax
import jax.numpy as jnp
from jax import lax
from jax.experimental import pallas as pl
from jax.experimental.pallas import tpu as pltpu
from jax.sharding import PartitionSpec as P

HD = 64
EPS = 1e-05
ROPE_BASE = 500000.0
BIG = 1e30
LOG2E = 1.4426950408889634
MESH = pl.DeviceIdType.MESH


def gathered_total(shard, axis):
    return lax.all_gather(shard, axis).astype(jnp.float32).sum(0)


def in_blocks(shard, dim, peers):
    before, after = (shard.shape[:dim], shard.shape[dim + 1 :])
    return jnp.moveaxis(shard.reshape(*before, peers, -1, *after), dim, 0)


def sum_at_owner(shard, axis, dim):
    peers = lax.axis_size(axis)
    parts = lax.all_to_all(in_blocks(shard, dim, peers), axis, 0, 0, tiled=True)
    return jnp.sum(parts.astype(jnp.float32), axis=0)


def origin(flow, major, minor, x):
    if flow == 0:
        return minor * 8 + major * 2 + x
    return major * 8 + minor * 2 + x


def plane(i, major, x):
    k = i // 2
    step = (3 * k + 3 * (k // 2) + 2 * (k // 3)) % 4
    return (major + step) % 4, (x + i) % 2


def attention_kernel(
    tok, gain, wq, wk, wv, cos, sin, bias, diag, out,
    normed, kv, qp, m_ref, l_ref, acc, send_sem, recv_sem,
):
    b = lax.axis_index("blk")
    z, y, x = b // 8, (b // 2) % 4, b % 2
    coords = ((y, z), (z, y))

    barrier = pltpu.get_barrier_semaphore()
    peers = [origin(0, y, z, (x + 1) % 2)]
    peers += [origin(0, (y + d) % 4, z, x) for d in (1, 3)]
    peers += [origin(0, y, (z + d) % 4, x) for d in (1, 3)]
    for peer in peers:
        pl.semaphore_signal(barrier, inc=1, device_id={"blk": peer}, device_id_type=MESH)

    rows = 64

    def norm_rows(r, _):
        at = pl.ds(pl.multiple_of(r * rows, rows), rows)
        t = tok[at, :].astype(jnp.float32)
        scale = lax.rsqrt(jnp.mean(t * t, axis=-1, keepdims=True) + EPS)
        normed[at, :] = (t * scale * gain[...]).astype(jnp.bfloat16)
        return 0

    lax.fori_loop(0, 256 // rows, norm_rows, 0)

    c = cos[...]
    s = sin[...]

    def rotated(u):
        a, h = u[0:32], u[32:64]
        return jnp.concatenate([a * c - h * s, h * c + a * s], axis=0)

    k = jnp.dot(normed[...], wk[...], preferred_element_type=jnp.float32).T
    kt = jnp.concatenate([rotated(k[0:64]), rotated(k[64:128])], axis=0)
    kn = kt.T.astype(jnp.bfloat16)
    v = jnp.dot(normed[...], wv[...], preferred_element_type=jnp.float32).T.astype(jnp.bfloat16)
    for f in range(2):
        kv[2 * b + f, 0:128, :] = kn[128 * f : 128 * f + 128, :]
        kv[2 * b + f, 128:256, :] = v[:, 128 * f : 128 * f + 128]

    pl.semaphore_wait(barrier, 5)

    def copy(f, org, dest, i, which):
        unit = 2 * org + f
        return pltpu.make_async_remote_copy(
            src_ref=kv.at[unit], dst_ref=kv.at[unit],
            send_sem=send_sem.at[f, i, which], recv_sem=recv_sem.at[unit],
            device_id={"blk": dest}, device_id_type=MESH,
        )

    def arrived(f, org):
        unit = 2 * org + f
        pltpu.make_async_remote_copy(
            src_ref=kv.at[unit], dst_ref=kv.at[unit],
            send_sem=send_sem.at[f, 0, 0], recv_sem=recv_sem.at[unit],
            device_id={"blk": peers[0]}, device_id_type=MESH,
        ).wait_recv()

    for f in range(2):
        major, minor = coords[f]
        copy(f, b, origin(f, major, minor, (x + 1) % 2), 0, 4).start()
    for f in range(2):
        major, minor = coords[f]
        copy(f, b, origin(f, (major + 1) % 4, minor, x), 0, 2).start()
        copy(f, b, origin(f, (major + 3) % 4, minor, x), 0, 3).start()
    for f in range(2):
        major, minor = coords[f]
        copy(f, b, origin(f, major, (minor + 1) % 4, x), 0, 0).start()
        copy(f, b, origin(f, major, (minor + 3) % 4, x), 0, 1).start()

    zero = jnp.zeros((64, 256), jnp.bfloat16)
    for half in range(2):
        q = jnp.dot(
            normed[...], wq[:, 256 * half : 256 * half + 256], preferred_element_type=jnp.float32
        ).T
        for n in range(4):
            u = (rotated(q[64 * n : 64 * n + 64]) * (HD**-0.5 * LOG2E)).astype(jnp.bfloat16)
            top, low = (u, zero) if half == 0 else (zero, u)
            qp[half, n, 0:64, :] = top
            qp[half, n, 64:128, :] = low

    def attend(ja, jb, first):
        ka, kb = kv[ja, 0:128, :], kv[jb, 0:128, :]
        if not first:
            ba, bb = bias[pl.ds(ja, 1), :], bias[pl.ds(jb, 1), :]
        for g in range(2):
            va = kv[ja, 128 + 64 * g : 192 + 64 * g, :]
            vb = kv[jb, 128 + 64 * g : 192 + 64 * g, :]
            vt = jnp.concatenate([va, vb], axis=1)
            for n in range(4):
                sa = jnp.dot(ka, qp[g, n], preferred_element_type=jnp.float32)
                sb = jnp.dot(kb, qp[g, n], preferred_element_type=jnp.float32)
                row = 4 * g + n
                if first:
                    sa = sa + diag[0:128, :]
                    sb = sb + diag[128:256, :]
                    new = jnp.maximum(
                        jnp.max(sa, axis=0, keepdims=True), jnp.max(sb, axis=0, keepdims=True)
                    )
                    pa, pb = jnp.exp2(sa - new), jnp.exp2(sb - new)
                else:
                    old = m_ref[row : row + 1, :]
                    new = jnp.maximum(
                        old,
                        jnp.maximum(
                            jnp.max(sa, axis=0, keepdims=True) - ba,
                            jnp.max(sb, axis=0, keepdims=True) - bb,
                        ),
                    )
                    pa, pb = jnp.exp2(sa - (new + ba)), jnp.exp2(sb - (new + bb))
                total = jnp.sum(pa, axis=0, keepdims=True) + jnp.sum(pb, axis=0, keepdims=True)
                p = jnp.concatenate([pa, pb], axis=0).astype(jnp.bfloat16)
                o = jnp.dot(vt, p, preferred_element_type=jnp.float32)
                if first:
                    l_ref[row : row + 1, :] = total
                    acc[64 * row : 64 * row + 64, :] = o
                else:
                    factor = jnp.exp2(old - new)
                    l_ref[row : row + 1, :] = l_ref[row : row + 1, :] * factor + total
                    acc[64 * row : 64 * row + 64, :] = acc[64 * row : 64 * row + 64, :] * factor + o
                m_ref[row : row + 1, :] = new

    attend(2 * b, 2 * b + 1, True)

    def first_plane(i, _):
        orgs = []
        for f in range(2):
            major, minor = coords[f]
            pp, xx = plane(i, major, x)
            org = origin(f, pp, minor, xx)
            orgs.append(org)
            arrived(f, org)

            @pl.when((i == 1) | (i == 2))
            def _():
                copy(f, org, origin(f, (major + 1) % 4, minor, x), i, 2).start()

            @pl.when((i == 1) | (i == 5))
            def _():
                copy(f, org, origin(f, (major + 3) % 4, minor, x), i, 3).start()

            copy(f, org, origin(f, major, (minor + 1) % 4, x), i, 0).start()
            copy(f, org, origin(f, major, (minor + 3) % 4, x), i, 1).start()
        attend(2 * orgs[0], 2 * orgs[1] + 1, False)
        return 0

    lax.fori_loop(1, 8, first_plane, 0)

    def near(n, _):
        i, back = n // 2, (n + 1) % 2
        orgs = []
        for f in range(2):
            major, minor = coords[f]
            pp, xx = plane(i, major, x)
            org = origin(f, pp, (minor + 1 + 2 * back) % 4, xx)
            orgs.append(org)
            arrived(f, org)

            @pl.when(i % 2 == 1 - back)
            def _():
                copy(f, org, origin(f, major, (minor + 3 + 2 * back) % 4, x), i, 5).start()

        attend(2 * orgs[0], 2 * orgs[1] + 1, False)
        return 0

    lax.fori_loop(0, 16, near, 0)

    def far(i, _):
        orgs = []
        for f in range(2):
            major, minor = coords[f]
            pp, xx = plane(i, major, x)
            org = origin(f, pp, (minor + 2) % 4, xx)
            orgs.append(org)
            arrived(f, org)
        attend(2 * orgs[0], 2 * orgs[1] + 1, False)
        return 0

    lax.fori_loop(0, 8, far, 0)

    for n in range(8):
        inv = 1.0 / l_ref[n : n + 1, :]
        out[:, 64 * n : 64 * n + 64] = (acc[64 * n : 64 * n + 64, :] * inv).T.astype(jnp.bfloat16)

    def sent(i, _):
        for f in range(2):
            for which in (0, 1, 5):
                copy(f, b, peers[0], i, which).wait_send()
        return 0

    lax.fori_loop(0, 8, sent, 0)
    for f in range(2):
        for i, which in ((0, 4), (0, 2), (0, 3), (1, 2), (1, 3), (2, 2), (5, 3)):
            copy(f, b, peers[0], i, which).wait_send()


def attention(tok, gain, wq, wk, wv, cos, sin, bias, diag):
    vmem = pl.BlockSpec(memory_space=pltpu.VMEM)
    return pl.pallas_call(
        attention_kernel,
        out_shape=jax.ShapeDtypeStruct((256, 512), jnp.bfloat16),
        in_specs=[vmem] * 9,
        out_specs=vmem,
        scratch_shapes=[
            pltpu.VMEM((256, 2048), jnp.bfloat16),
            pltpu.VMEM((64, 256, 128), jnp.bfloat16),
            pltpu.VMEM((2, 4, 128, 256), jnp.bfloat16),
            pltpu.VMEM((8, 256), jnp.float32),
            pltpu.VMEM((8, 256), jnp.float32),
            pltpu.VMEM((512, 256), jnp.float32),
            pltpu.SemaphoreType.DMA((2, 8, 6)),
            pltpu.SemaphoreType.DMA((64,)),
        ],
        compiler_params=pltpu.CompilerParams(
            collective_id=0, has_side_effects=True, vmem_limit_bytes=48 * 1024 * 1024
        ),
        name="attention",
    )(tok, gain, wq, wk, wv, cos, sin, bias, diag)


def local(tokens, order, gain_attn, gain_ffn, w_query, w_key, w_value, w_out, w_gate, w_up, w_down):
    tok_rows, model_width = tokens.shape
    half_rows = tok_rows // 2
    b = lax.axis_index("blk")
    own = lax.dynamic_slice_in_dim(order, 2 * b, 2)
    block_of = jnp.repeat(own, half_rows)
    pos = block_of * half_rows + jnp.arange(tok_rows, dtype=jnp.int32) % half_rows
    freq = ROPE_BASE ** (-(jnp.arange(HD // 2, dtype=jnp.float32) * 2.0 / HD))
    angle = freq[:, None] * pos.astype(jnp.float32)[None, :]
    bias = jnp.where(order[:, None] > block_of[None, :], BIG, 0.0).astype(jnp.float32)
    diag = jnp.where(pos[:, None] <= pos[None, :], 0.0, -BIG).astype(jnp.float32)
    heads = attention(
        tokens, gain_attn[None, :], w_query, w_key, w_value, jnp.cos(angle), jnp.sin(angle), bias, diag
    )
    tokens_wide = tokens.astype(jnp.float32)
    partial_value = jnp.dot(heads, w_out, preferred_element_type=jnp.float32)
    share = model_width // lax.axis_size("tp")
    col_start = lax.axis_index("tp") * share
    attention_sum = gathered_total(partial_value.astype(jnp.bfloat16), "tp").astype(jnp.float32)
    resid_full = tokens_wide + attention_sum
    normed_ffn = (
        resid_full
        * lax.rsqrt(jnp.mean(resid_full * resid_full, axis=-1, keepdims=True) + EPS)
        * gain_ffn
    ).astype(jnp.bfloat16)
    gate = jnp.dot(normed_ffn, w_gate, preferred_element_type=jnp.float32)
    up_proj = jnp.dot(normed_ffn, w_up, preferred_element_type=jnp.float32)
    residual = lax.dynamic_slice_in_dim(resid_full, col_start, share, 1)
    hidden = (jax.nn.silu(gate) * up_proj).astype(jnp.bfloat16)
    down = jnp.dot(hidden, w_down, preferred_element_type=jnp.float32)
    feed = sum_at_owner(down.astype(jnp.bfloat16), "tp", 1)
    return (residual + feed).astype(jnp.bfloat16)


def solution(mesh):
    placed = (
        P("blk", None),
        P(),
        P(),
        P(),
        P(None, "tp"),
        P(None, "tp"),
        P(None, "tp"),
        P("tp", None),
        P(None, "tp"),
        P(None, "tp"),
        P("tp", None),
    )
    return jax.shard_map(
        local, mesh=mesh, in_specs=placed, out_specs=P("blk", "tp"), check_vma=False
    )
```

```python
import jax
import jax.numpy as jnp
from jax import lax
from jax.experimental import pallas as pl
from jax.experimental.pallas import tpu as pltpu
from jax.sharding import PartitionSpec as P

HD = 64
SHARE = 512
CHUNKS = 2
ROWS = 256 // CHUNKS
EPS = 1e-05
ROPE_BASE = 500000.0
BIG = 1e30
LOG2E = 1.4426950408889634
MESH = pl.DeviceIdType.MESH


def origin(flow, major, minor, x):
    if flow == 0:
        return minor * 8 + major * 2 + x
    return major * 8 + minor * 2 + x


def plane(i, major, x):
    k = i // 2
    step = (3 * k + 3 * (k // 2) + 2 * (k // 3)) % 4
    return (major + step) % 4, (x + i) % 2


def layer_kernel(
    tok_hbm, gain, wq_hbm, wk_hbm, wv_hbm, cos, sin, bias, diag, gain2, wo_hbm, wg_hbm, wu_hbm, wd_hbm,
    out, tok, wq, wk, wv, wo, wg, wu, wd, heads, near_out, near_in, far_out, far_in, kept, resid,
    shares, hidden, load_sem, tail_send, tail_recv, normed, kv, qp, s_ref, mo_ref, f_ref, m_ref, l_ref, acc, send_sem, recv_sem,
):
    b = lax.axis_index("blk")
    z, y, x = b // 8, (b // 2) % 4, b % 2
    coords = ((y, z), (z, y))

    t = lax.axis_index("tp")
    core = t % 2
    twin = t + 1 - 2 * core
    across = (t + 2) % 4
    loads = [
        pltpu.make_async_copy(src, dst, load_sem.at[i])
        for i, (src, dst) in enumerate(
            ((tok_hbm, tok), (wk_hbm, wk), (wv_hbm, wv), (wq_hbm, wq))
            + ((wo_hbm, wo), (wg_hbm, wg), (wu_hbm, wu), (wd_hbm, wd))
        )
    ]
    for load in loads[:4]:
        load.start()
    barrier = pltpu.get_barrier_semaphore()
    for peer in (twin, across):
        pl.semaphore_signal(barrier, inc=1, device_id={"tp": peer}, device_id_type=MESH)
    peers = [origin(0, y, z, (x + 1) % 2)]
    peers += [origin(0, (y + d) % 4, z, x) for d in (1, 3)]
    peers += [origin(0, y, (z + d) % 4, x) for d in (1, 3)]
    for peer in peers:
        pl.semaphore_signal(barrier, inc=1, device_id={"blk": peer}, device_id_type=MESH)

    rows = 64
    loads[0].wait()

    def norm_rows(r, _):
        at = pl.ds(pl.multiple_of(r * rows, rows), rows)
        t = tok[at, :].astype(jnp.float32)
        scale = lax.rsqrt(jnp.mean(t * t, axis=-1, keepdims=True) + EPS)
        normed[at, :] = (t * scale * gain[...]).astype(jnp.bfloat16)
        return 0

    lax.fori_loop(0, 256 // rows, norm_rows, 0)

    c = cos[...]
    s = sin[...]

    def rotated(u):
        a, h = u[0:32], u[32:64]
        return jnp.concatenate([a * c - h * s, h * c + a * s], axis=0)

    loads[1].wait()
    loads[2].wait()
    k = jnp.dot(normed[...], wk[...], preferred_element_type=jnp.float32).T
    kt = jnp.concatenate([rotated(k[0:64]), rotated(k[64:128])], axis=0)
    kn = kt.T.astype(jnp.bfloat16)
    v = jnp.dot(normed[...], wv[...], preferred_element_type=jnp.float32).T.astype(jnp.bfloat16)
    for f in range(2):
        kv[2 * b + f, 0:128, :] = kn[128 * f : 128 * f + 128, :]
        kv[2 * b + f, 128:256, :] = v[:, 128 * f : 128 * f + 128]

    pl.semaphore_wait(barrier, 7)

    def copy(f, org, dest, i, which):
        unit = 2 * org + f
        return pltpu.make_async_remote_copy(
            src_ref=kv.at[unit], dst_ref=kv.at[unit],
            send_sem=send_sem.at[f, i, which], recv_sem=recv_sem.at[unit],
            device_id={"blk": dest}, device_id_type=MESH,
        )

    def arrived(f, org):
        unit = 2 * org + f
        pltpu.make_async_remote_copy(
            src_ref=kv.at[unit], dst_ref=kv.at[unit],
            send_sem=send_sem.at[f, 0, 0], recv_sem=recv_sem.at[unit],
            device_id={"blk": peers[0]}, device_id_type=MESH,
        ).wait_recv()

    for f in range(2):
        major, minor = coords[f]
        copy(f, b, origin(f, major, minor, (x + 1) % 2), 0, 4).start()
    for f in range(2):
        major, minor = coords[f]
        copy(f, b, origin(f, (major + 1) % 4, minor, x), 0, 2).start()
        copy(f, b, origin(f, (major + 3) % 4, minor, x), 0, 3).start()
    for f in range(2):
        major, minor = coords[f]
        copy(f, b, origin(f, major, (minor + 1) % 4, x), 0, 0).start()
        copy(f, b, origin(f, major, (minor + 3) % 4, x), 0, 1).start()

    loads[3].wait()
    for load in loads[4:]:
        load.start()
    zero = jnp.zeros((64, 256), jnp.bfloat16)
    for half in range(2):
        q = jnp.dot(
            normed[...], wq[:, 256 * half : 256 * half + 256], preferred_element_type=jnp.float32
        ).T
        for n in range(4):
            u = (rotated(q[64 * n : 64 * n + 64]) * (HD**-0.5 * LOG2E)).astype(jnp.bfloat16)
            top, low = (u, zero) if half == 0 else (zero, u)
            qp[half, n, 0:64, :] = top
            qp[half, n, 64:128, :] = low

    def weigh(row, ja, jb, first):
        g, n = row // 4, row % 4
        pa = jnp.exp2(s_ref[row, 0:128, :] - mo_ref[0, row : row + 1, :])
        pb = jnp.exp2(s_ref[row, 128:256, :] - mo_ref[1, row : row + 1, :])
        total = jnp.sum(pa, axis=0, keepdims=True) + jnp.sum(pb, axis=0, keepdims=True)
        p = jnp.concatenate([pa, pb], axis=0).astype(jnp.bfloat16)
        va = kv[ja, 128 + 64 * g : 192 + 64 * g, :]
        vb = kv[jb, 128 + 64 * g : 192 + 64 * g, :]
        o = jnp.dot(jnp.concatenate([va, vb], axis=1), p, preferred_element_type=jnp.float32)
        if first:
            l_ref[row : row + 1, :] = total
            acc[64 * row : 64 * row + 64, :] = o
        else:
            factor = f_ref[row : row + 1, :]
            l_ref[row : row + 1, :] = l_ref[row : row + 1, :] * factor + total
            acc[64 * row : 64 * row + 64, :] = acc[64 * row : 64 * row + 64, :] * factor + o

    def score(row, ja, jb, first):
        g, n = row // 4, row % 4
        sa = jnp.dot(kv[ja, 0:128, :], qp[g, n], preferred_element_type=jnp.float32)
        sb = jnp.dot(kv[jb, 0:128, :], qp[g, n], preferred_element_type=jnp.float32)
        if first:
            sa = sa + diag[0:128, :]
            sb = sb + diag[128:256, :]
        s_ref[row, 0:128, :] = sa
        s_ref[row, 128:256, :] = sb
        ma, mb = jnp.max(sa, axis=0, keepdims=True), jnp.max(sb, axis=0, keepdims=True)
        if first:
            new = jnp.maximum(ma, mb)
            mo_ref[0, row : row + 1, :] = new
            mo_ref[1, row : row + 1, :] = new
        else:
            ba, bb = bias[pl.ds(ja, 1), :], bias[pl.ds(jb, 1), :]
            old = m_ref[row : row + 1, :]
            new = jnp.maximum(old, jnp.maximum(ma - ba, mb - bb))
            f_ref[row : row + 1, :] = jnp.exp2(old - new)
            mo_ref[0, row : row + 1, :] = new + ba
            mo_ref[1, row : row + 1, :] = new + bb
        m_ref[row : row + 1, :] = new

    def attend(before, now):
        for row in range(8):
            weigh(row, *before, False)
            score(row, *now, False)
        return now

    for row in range(8):
        score(row, 2 * b, 2 * b + 1, True)
    for row in range(8):
        l_ref[row : row + 1, :] = jnp.zeros((1, 256), jnp.float32)
        acc[64 * row : 64 * row + 64, :] = jnp.zeros((64, 256), jnp.float32)
        f_ref[row : row + 1, :] = jnp.zeros((1, 256), jnp.float32)
    held = (2 * b, 2 * b + 1)

    def first_plane(i, held):
        orgs = []
        for f in range(2):
            major, minor = coords[f]
            pp, xx = plane(i, major, x)
            org = origin(f, pp, minor, xx)
            orgs.append(org)
            arrived(f, org)

            @pl.when((i == 1) | (i == 2))
            def _():
                copy(f, org, origin(f, (major + 1) % 4, minor, x), i, 2).start()

            @pl.when((i == 1) | (i == 5))
            def _():
                copy(f, org, origin(f, (major + 3) % 4, minor, x), i, 3).start()

            copy(f, org, origin(f, major, (minor + 1) % 4, x), i, 0).start()
            copy(f, org, origin(f, major, (minor + 3) % 4, x), i, 1).start()
        return attend(held, (2 * orgs[0], 2 * orgs[1] + 1))

    held = lax.fori_loop(1, 8, first_plane, held)

    def near(n, held):
        i, back = n // 2, (n + 1) % 2
        orgs = []
        for f in range(2):
            major, minor = coords[f]
            pp, xx = plane(i, major, x)
            org = origin(f, pp, (minor + 1 + 2 * back) % 4, xx)
            orgs.append(org)
            arrived(f, org)

            @pl.when(i % 2 == 1 - back)
            def _():
                copy(f, org, origin(f, major, (minor + 3 + 2 * back) % 4, x), i, 5).start()

        return attend(held, (2 * orgs[0], 2 * orgs[1] + 1))

    held = lax.fori_loop(0, 16, near, held)

    def far(i, held):
        orgs = []
        for f in range(2):
            major, minor = coords[f]
            pp, xx = plane(i, major, x)
            org = origin(f, pp, (minor + 2) % 4, xx)
            orgs.append(org)
            arrived(f, org)
        return attend(held, (2 * orgs[0], 2 * orgs[1] + 1))

    held = lax.fori_loop(0, 8, far, held)
    for row in range(8):
        weigh(row, *held, False)

    for n in range(8):
        inv = 1.0 / l_ref[n : n + 1, :]
        heads[:, 64 * n : 64 * n + 64] = (acc[64 * n : 64 * n + 64, :] * inv).T.astype(jnp.bfloat16)

    def sent(i, _):
        for f in range(2):
            for which in (0, 1, 5):
                copy(f, b, peers[0], i, which).wait_send()
        return 0

    lax.fori_loop(0, 8, sent, 0)
    for f in range(2):
        for i, which in ((0, 4), (0, 2), (0, 3), (1, 2), (1, 3), (2, 2), (5, 3)):
            copy(f, b, peers[0], i, which).wait_send()

    def tail_copy(stage, r, src, dst, peer):
        return pltpu.make_async_remote_copy(
            src_ref=src, dst_ref=dst,
            send_sem=tail_send.at[stage, r], recv_sem=tail_recv.at[stage, r],
            device_id={"tp": peer}, device_id_type=MESH,
        )

    def columns(c):
        return pl.ds(pl.multiple_of(c * SHARE, SHARE), SHARE)

    def project(stage, r, lhs, w):
        for j, c in enumerate((1 - core, 3 - core)):
            part = jnp.dot(lhs, w[:, columns(c)], preferred_element_type=jnp.float32)
            near_out[stage, r, j] = part.astype(jnp.bfloat16)
        tail_copy(2 * stage, r, near_out.at[stage, r], near_in.at[stage, r], twin).start()
        for j, c in enumerate((across, t)):
            kept[r, j] = jnp.dot(lhs, w[:, columns(c)], preferred_element_type=jnp.float32)

    def cross(stage, r):
        tail_copy(2 * stage, r, near_out.at[stage, r], near_in.at[stage, r], twin).wait()
        far = 1 - t // 2
        far_out[stage, r] = (kept[r, 0] + near_in[stage, r, far].astype(jnp.float32)).astype(jnp.bfloat16)
        tail_copy(2 * stage + 1, r, far_out.at[stage, r], far_in.at[stage, r], across).start()
        kept[r, 1] = kept[r, 1] + near_in[stage, r, 1 - far].astype(jnp.float32)

    def total(stage, r):
        tail_copy(2 * stage + 1, r, far_out.at[stage, r], far_in.at[stage, r], across).wait()
        return kept[r, 1] + far_in[stage, r].astype(jnp.float32)

    def share_copy(stage, r, slot, peer):
        return tail_copy(stage, r, shares.at[r, slot], shares.at[r, slot], peer)

    loads[4].wait()
    for r in range(CHUNKS):
        project(0, r, heads[ROWS * r : ROWS * r + ROWS, :], wo)
    for r in range(CHUNKS):
        cross(0, r)
    for r in range(CHUNKS):
        at = slice(ROWS * r, ROWS * r + ROWS)
        own = tok[at, columns(t)].astype(jnp.float32) + total(0, r)
        resid[at, :] = own
        shares[r, t] = own.astype(jnp.bfloat16)
        share_copy(4, r, t, across).start()
        share_copy(5, r, t, twin).start()
    for load in loads[5:]:
        load.wait()

    def feed_forward(r):
        share_copy(4, r, across, across).wait_recv()
        share_copy(6, r, across, twin).start()
        share_copy(5, r, twin, twin).wait_recv()
        share_copy(6, r, (twin + 2) % 4, twin).wait_recv()
        squares = jnp.zeros((ROWS, 1), jnp.float32)
        for c in range(4):
            u = shares[r, c].astype(jnp.float32)
            squares = squares + jnp.sum(u * u, axis=-1, keepdims=True)
        scale = lax.rsqrt(squares * (1.0 / (4 * SHARE)) + EPS)
        for c in range(4):
            u = shares[r, c].astype(jnp.float32)
            at = slice(SHARE * c, SHARE * c + SHARE)
            normed[ROWS * r : ROWS * r + ROWS, at] = (u * scale * gain2[:, at]).astype(jnp.bfloat16)

        def units(n, _):
            at = pl.ds(pl.multiple_of(n * 256, 256), 256)
            u = normed[ROWS * r : ROWS * r + ROWS, :]
            gate = jnp.dot(u, wg[:, at], preferred_element_type=jnp.float32)
            up = jnp.dot(u, wu[:, at], preferred_element_type=jnp.float32)
            hidden[r, :, at] = (gate / (1.0 + jnp.exp(-gate)) * up).astype(jnp.bfloat16)
            return 0

        lax.fori_loop(0, 8, units, 0)
        project(1, r, hidden[r], wd)

    for r in range(CHUNKS):
        feed_forward(r)
        if r > 0:
            cross(1, r - 1)
    cross(1, CHUNKS - 1)
    for r in range(CHUNKS):
        at = slice(ROWS * r, ROWS * r + ROWS)
        out[at, :] = (resid[at, :] + total(1, r)).astype(jnp.bfloat16)
    for r in range(CHUNKS):
        share_copy(4, r, t, across).wait_send()
        share_copy(5, r, t, twin).wait_send()
        share_copy(6, r, across, twin).wait_send()


def layer(tok, gain, wq, wk, wv, cos, sin, bias, diag, gain2, wo, wg, wu, wd):
    vmem = pl.BlockSpec(memory_space=pltpu.VMEM)
    hbm = pl.BlockSpec(memory_space=pl.ANY)
    bf16, f32 = jnp.bfloat16, jnp.float32
    return pl.pallas_call(
        layer_kernel,
        out_shape=jax.ShapeDtypeStruct((256, SHARE), bf16),
        in_specs=[hbm, vmem, hbm, hbm, hbm, vmem, vmem, vmem, vmem, vmem, hbm, hbm, hbm, hbm],
        out_specs=vmem,
        scratch_shapes=[
            pltpu.VMEM((256, 2048), bf16),
            pltpu.VMEM((2048, 512), bf16),
            pltpu.VMEM((2048, 128), bf16),
            pltpu.VMEM((2048, 128), bf16),
            pltpu.VMEM((512, 2048), bf16),
            pltpu.VMEM((2048, 2048), bf16),
            pltpu.VMEM((2048, 2048), bf16),
            pltpu.VMEM((2048, 2048), bf16),
            pltpu.VMEM((256, 512), bf16),
            pltpu.VMEM((2, CHUNKS, 2, ROWS, SHARE), bf16),
            pltpu.VMEM((2, CHUNKS, 2, ROWS, SHARE), bf16),
            pltpu.VMEM((2, CHUNKS, ROWS, SHARE), bf16),
            pltpu.VMEM((2, CHUNKS, ROWS, SHARE), bf16),
            pltpu.VMEM((CHUNKS, 2, ROWS, SHARE), f32),
            pltpu.VMEM((256, SHARE), f32),
            pltpu.VMEM((CHUNKS, 4, ROWS, SHARE), bf16),
            pltpu.VMEM((CHUNKS, ROWS, 2048), bf16),
            pltpu.SemaphoreType.DMA((8,)),
            pltpu.SemaphoreType.DMA((7, CHUNKS)),
            pltpu.SemaphoreType.DMA((7, CHUNKS)),
            pltpu.VMEM((256, 2048), bf16),
            pltpu.VMEM((64, 256, 128), bf16),
            pltpu.VMEM((2, 4, 128, 256), bf16),
            pltpu.VMEM((8, 256, 256), f32),
            pltpu.VMEM((2, 8, 256), f32),
            pltpu.VMEM((8, 256), f32),
            pltpu.VMEM((8, 256), f32),
            pltpu.VMEM((8, 256), f32),
            pltpu.VMEM((512, 256), f32),
            pltpu.SemaphoreType.DMA((2, 8, 6)),
            pltpu.SemaphoreType.DMA((64,)),
        ],
        compiler_params=pltpu.CompilerParams(
            collective_id=0, has_side_effects=True, vmem_limit_bytes=62 * 1024 * 1024
        ),
        name="layer",
    )(tok, gain, wq, wk, wv, cos, sin, bias, diag, gain2, wo, wg, wu, wd)


def local(tokens, order, gain_attn, gain_ffn, w_query, w_key, w_value, w_out, w_gate, w_up, w_down):
    tok_rows = tokens.shape[0]
    half_rows = tok_rows // 2
    b = lax.axis_index("blk")
    own = lax.dynamic_slice_in_dim(order, 2 * b, 2)
    block_of = jnp.repeat(own, half_rows)
    pos = block_of * half_rows + jnp.arange(tok_rows, dtype=jnp.int32) % half_rows
    freq = ROPE_BASE ** (-(jnp.arange(HD // 2, dtype=jnp.float32) * 2.0 / HD))
    angle = freq[:, None] * pos.astype(jnp.float32)[None, :]
    bias = jnp.where(order[:, None] > block_of[None, :], BIG, 0.0).astype(jnp.float32)
    diag = jnp.where(pos[:, None] <= pos[None, :], 0.0, -BIG).astype(jnp.float32)
    return layer(
        tokens, gain_attn[None, :], w_query, w_key, w_value, jnp.cos(angle), jnp.sin(angle), bias, diag,
        gain_ffn[None, :], w_out, w_gate, w_up, w_down,
    )


def solution(mesh):
    placed = (
        P("blk", None),
        P(),
        P(),
        P(),
        P(None, "tp"),
        P(None, "tp"),
        P(None, "tp"),
        P("tp", None),
        P(None, "tp"),
        P(None, "tp"),
        P("tp", None),
    )
    return jax.shard_map(
        local, mesh=mesh, in_specs=placed, out_specs=P("blk", "tp"), check_vma=False
    )
```

```python
import jax
import jax.numpy as jnp
import numpy as np
from jax import lax
from jax.experimental import pallas as pl
from jax.experimental.pallas import tpu as pltpu
from jax.sharding import PartitionSpec as P

HD = 64
SHARE = 512
CHUNKS = 2
ROWS = 256 // CHUNKS
PIECE = 64
UNITS = 512
EPS = 1e-05
ROPE_BASE = 500000.0
BIG = 1e30
LOG2E = 1.4426950408889634
MESH = pl.DeviceIdType.MESH


def rope_table():
    freq = ROPE_BASE ** (-np.arange(HD // 2) * 2.0 / HD)[:, None]
    within = freq * np.arange(128)[None, :]
    starts = freq * (128.0 * np.arange(128))[None, :]
    return np.concatenate([np.cos(within), np.sin(within), np.cos(starts), np.sin(starts)]).astype(np.float32)


def origin(flow, major, minor, x):
    if flow == 0:
        return minor * 8 + major * 2 + x
    return major * 8 + minor * 2 + x


def plane(i, major, x):
    k = i // 2
    step = (3 * k + 3 * (k // 2) + 2 * (k // 3)) % 4
    return (major + step) % 4, (x + i) % 2


def layer_kernel(
    tok_hbm, order, gain, wq_hbm, wk_hbm, wv_hbm, tab, gain2, wo_hbm, wg_hbm, wu_hbm, wd_hbm,
    out, diag, blocks, gated, squares, tok, wq, wk, wv, wo, wg, wu, wd, heads, near_out, near_in, far_out, far_in, kept, resid,
    shares, hidden, load_sem, tail_send, tail_recv, normed, kv, qp, s_ref, mo_ref, f_ref, m_ref, l_ref, acc, send_sem, recv_sem,
):
    b = lax.axis_index("blk")
    z, y, x = b // 8, (b // 2) % 4, b % 2
    coords = ((y, z), (z, y))

    t = lax.axis_index("tp")
    core = t % 2
    twin = t + 1 - 2 * core
    across = (t + 2) % 4
    loads = [
        pltpu.make_async_copy(src, dst, load_sem.at[i])
        for i, (src, dst) in enumerate(
            ((tok_hbm, tok), (wk_hbm, wk), (wv_hbm, wv), (wq_hbm, wq))
            + ((wo_hbm, wo), (wg_hbm, wg), (wu_hbm, wu), (wd_hbm, wd))
        )
    ]
    for load in loads[:4]:
        load.start()
    barrier = pltpu.get_barrier_semaphore()
    for peer in (twin, across):
        pl.semaphore_signal(barrier, inc=1, device_id={"tp": peer}, device_id_type=MESH)
    peers = [origin(0, y, z, (x + 1) % 2)]
    peers += [origin(0, (y + d) % 4, z, x) for d in (1, 3)]
    peers += [origin(0, y, (z + d) % 4, x) for d in (1, 3)]
    for peer in peers:
        pl.semaphore_signal(barrier, inc=1, device_id={"blk": peer}, device_id_type=MESH)

    rows = 64
    loads[0].wait()

    def norm_rows(r, _):
        at = pl.ds(pl.multiple_of(r * rows, rows), rows)
        t = tok[at, :].astype(jnp.float32)
        scale = lax.rsqrt(jnp.mean(t * t, axis=-1, keepdims=True) + EPS)
        normed[at, :] = (t * scale * gain[...]).astype(jnp.bfloat16)
        return 0

    lax.fori_loop(0, 256 // rows, norm_rows, 0)

    first, second = order[2 * b], order[2 * b + 1]
    lane = lax.broadcasted_iota(jnp.int32, (32, 128), 1)
    cosines, sines = [], []
    for block in (first, second):
        ca = jnp.sum(jnp.where(lane == block, tab[64:96, :], 0.0), axis=1, keepdims=True)
        sa = jnp.sum(jnp.where(lane == block, tab[96:128, :], 0.0), axis=1, keepdims=True)
        cosines.append(ca * tab[0:32, :] - sa * tab[32:64, :])
        sines.append(sa * tab[0:32, :] + ca * tab[32:64, :])
    c = jnp.concatenate(cosines, axis=1)
    s = jnp.concatenate(sines, axis=1)

    def rotated(u):
        a, h = u[0:32], u[32:64]
        return jnp.concatenate([a * c - h * s, h * c + a * s], axis=0)

    loads[1].wait()
    loads[2].wait()
    k = jnp.dot(normed[...], wk[...], preferred_element_type=jnp.float32).T
    kt = jnp.concatenate([rotated(k[0:64]), rotated(k[64:128])], axis=0)
    kn = kt.T.astype(jnp.bfloat16)
    v = jnp.dot(normed[...], wv[...], preferred_element_type=jnp.float32).T.astype(jnp.bfloat16)
    for f in range(2):
        kv[2 * b + f, 0:128, :] = kn[128 * f : 128 * f + 128, :]
        kv[2 * b + f, 128:256, :] = v[:, 128 * f : 128 * f + 128]

    pl.semaphore_wait(barrier, 7)

    def copy(f, org, dest, i, which):
        unit = 2 * org + f
        return pltpu.make_async_remote_copy(
            src_ref=kv.at[unit], dst_ref=kv.at[unit],
            send_sem=send_sem.at[f, i, which], recv_sem=recv_sem.at[unit],
            device_id={"blk": dest}, device_id_type=MESH,
        )

    def arrived(f, org):
        unit = 2 * org + f
        pltpu.make_async_remote_copy(
            src_ref=kv.at[unit], dst_ref=kv.at[unit],
            send_sem=send_sem.at[f, 0, 0], recv_sem=recv_sem.at[unit],
            device_id={"blk": peers[0]}, device_id_type=MESH,
        ).wait_recv()

    for f in range(2):
        major, minor = coords[f]
        copy(f, b, origin(f, major, minor, (x + 1) % 2), 0, 4).start()
    for f in range(2):
        major, minor = coords[f]
        copy(f, b, origin(f, (major + 1) % 4, minor, x), 0, 2).start()
        copy(f, b, origin(f, (major + 3) % 4, minor, x), 0, 3).start()
    for f in range(2):
        major, minor = coords[f]
        copy(f, b, origin(f, major, (minor + 1) % 4, x), 0, 0).start()
        copy(f, b, origin(f, major, (minor + 3) % 4, x), 0, 1).start()

    column = lax.broadcasted_iota(jnp.int32, (8, 256), 1)
    block_row = jnp.where(column < 128, first, second)
    blocks[...] = block_row
    place = block_row[0:1] * 128 + column[0:1] % 128
    for f, block in enumerate((first, second)):
        key_place = block * 128 + lax.broadcasted_iota(jnp.int32, (128, 256), 0)
        diag[128 * f : 128 * f + 128, :] = jnp.where(key_place <= place, 0.0, -BIG)

    loads[3].wait()
    for load in loads[4:]:
        load.start()
    zero = jnp.zeros((64, 256), jnp.bfloat16)
    for half in range(2):
        q = jnp.dot(
            normed[...], wq[:, 256 * half : 256 * half + 256], preferred_element_type=jnp.float32
        ).T
        for n in range(4):
            u = (rotated(q[64 * n : 64 * n + 64]) * (HD**-0.5 * LOG2E)).astype(jnp.bfloat16)
            top, low = (u, zero) if half == 0 else (zero, u)
            qp[half, n, 0:64, :] = top
            qp[half, n, 64:128, :] = low

    def weigh(row, ja, jb, first):
        g, n = row // 4, row % 4
        pa = jnp.exp2(s_ref[row, 0:128, :] - mo_ref[0, row : row + 1, :])
        pb = jnp.exp2(s_ref[row, 128:256, :] - mo_ref[1, row : row + 1, :])
        p = jnp.concatenate([pa, pb], axis=0).astype(jnp.bfloat16)
        va = kv[ja, 128 + 64 * g : 192 + 64 * g, :]
        vb = kv[jb, 128 + 64 * g : 192 + 64 * g, :]
        vt = jnp.concatenate([jnp.concatenate([va, vb], axis=1), jnp.ones((16, 256), jnp.bfloat16)], axis=0)
        o = jnp.dot(vt, p, preferred_element_type=jnp.float32)
        total, o = o[64:65], o[0:64]
        if first:
            l_ref[row : row + 1, :] = total
            acc[64 * row : 64 * row + 64, :] = o
        else:
            factor = f_ref[row : row + 1, :]
            l_ref[row : row + 1, :] = l_ref[row : row + 1, :] * factor + total
            acc[64 * row : 64 * row + 64, :] = acc[64 * row : 64 * row + 64, :] * factor + o

    def score(row, ja, jb, first):
        g, n = row // 4, row % 4
        sa = jnp.dot(kv[ja, 0:128, :], qp[g, n], preferred_element_type=jnp.float32)
        sb = jnp.dot(kv[jb, 0:128, :], qp[g, n], preferred_element_type=jnp.float32)
        if first:
            sa = sa + diag[0:128, :]
            sb = sb + diag[128:256, :]
        s_ref[row, 0:128, :] = sa
        s_ref[row, 128:256, :] = sb
        ma, mb = jnp.max(sa, axis=0, keepdims=True), jnp.max(sb, axis=0, keepdims=True)
        if first:
            new = jnp.maximum(ma, mb)
            mo_ref[0, row : row + 1, :] = new
            mo_ref[1, row : row + 1, :] = new
        else:
            ba = jnp.where(blocks[0:1, :] < order[ja], BIG, 0.0)
            bb = jnp.where(blocks[0:1, :] < order[jb], BIG, 0.0)
            old = m_ref[row : row + 1, :]
            new = jnp.maximum(old, jnp.maximum(ma - ba, mb - bb))
            f_ref[row : row + 1, :] = jnp.exp2(old - new)
            mo_ref[0, row : row + 1, :] = new + ba
            mo_ref[1, row : row + 1, :] = new + bb
        m_ref[row : row + 1, :] = new

    def attend(before, now):
        for row in range(8):
            weigh(row, *before, False)
            score(row, *now, False)
        return now

    for row in range(8):
        score(row, 2 * b, 2 * b + 1, True)
    for row in range(8):
        l_ref[row : row + 1, :] = jnp.zeros((1, 256), jnp.float32)
        acc[64 * row : 64 * row + 64, :] = jnp.zeros((64, 256), jnp.float32)
        f_ref[row : row + 1, :] = jnp.zeros((1, 256), jnp.float32)
    held = (2 * b, 2 * b + 1)

    def source(f, i, ds):
        major, minor = coords[f]
        pp, xx = plane(i, major, x)
        return origin(f, pp, (minor + ds) % 4, xx)

    def take_plane(i):
        for f in range(2):
            major, minor = coords[f]
            org = source(f, i, 0)
            arrived(f, org)

            @pl.when((i == 1) | (i == 2))
            def _():
                copy(f, org, origin(f, (major + 1) % 4, minor, x), i, 2).start()

            @pl.when((i == 1) | (i == 5))
            def _():
                copy(f, org, origin(f, (major + 3) % 4, minor, x), i, 3).start()

            copy(f, org, origin(f, major, (minor + 1) % 4, x), i, 0).start()
            copy(f, org, origin(f, major, (minor + 3) % 4, x), i, 1).start()

    def take_near(i, back, passing=False):
        for f in range(2):
            major, minor = coords[f]
            org = source(f, i, 1 + 2 * back)
            arrived(f, org)

            if passing:

                @pl.when((i // 2) % 2 == 1 - back)
                def _():
                    copy(f, org, origin(f, major, (minor + 3 + 2 * back) % 4, x), i, 5).start()

    def take_far(i, passing=False):
        for f in range(2):
            org = source(f, i, 2)
            arrived(f, org)
            if passing:
                copy(f, org, origin(f, *coords[f], (x + 1) % 2), i + 1, 5).start()

    def step(held, i, ds):
        return attend(held, (2 * source(0, i, ds), 2 * source(1, i, ds) + 1))

    def plane_even(k, held):
        take_plane(2 * k)
        return step(held, 2 * k, 0)

    def near_even(n, held):
        take_near(n // 2 * 2, (n + 1) % 2, True)

        @pl.when((n == 1) | (n == 2))
        def _():
            take_plane(5 * n - 4)

        @pl.when((n == 6) | (n == 7))
        def _():
            take_plane(2 * n - 9)

        return step(held, n // 2 * 2, 1 + 2 * ((n + 1) % 2))

    def far_even(k, held):
        take_far(2 * k, True)

        @pl.when(k == 2)
        def _():
            take_near(1, 1)
            take_near(1, 0)

        return step(held, 2 * k, 2)

    def plane_odd(k, held):
        @pl.when(k == 0)
        def _():
            take_plane(7)

        @pl.when((k == 1) | (k == 3))
        def _():
            take_near(k + 2, 1)
            take_near(k + 2, 0)

        return step(held, 2 * k + 1, 0)

    def near_odd(n, held):
        @pl.when(n == 2)
        def _():
            take_near(7, 1)
            take_near(7, 0)

        return step(held, n // 2 * 2 + 1, 1 + 2 * ((n + 1) % 2))

    def far_odd(k, held):
        take_far(2 * k + 1)
        return step(held, 2 * k + 1, 2)

    held = lax.fori_loop(1, 3, plane_even, held)
    held = lax.fori_loop(0, 8, near_even, held)
    held = step(held, 6, 0)
    held = lax.fori_loop(0, 4, far_even, held)
    held = lax.fori_loop(0, 4, plane_odd, held)
    held = lax.fori_loop(0, 8, near_odd, held)
    held = lax.fori_loop(0, 4, far_odd, held)
    for row in range(8):
        weigh(row, *held, False)

    for n in range(8):
        inv = 1.0 / l_ref[n : n + 1, :]
        heads[:, 64 * n : 64 * n + 64] = (acc[64 * n : 64 * n + 64, :] * inv).T.astype(jnp.bfloat16)

    def sent(i, _):
        for f in range(2):
            for which in (0, 1, 5):
                copy(f, b, peers[0], i, which).wait_send()
        return 0

    lax.fori_loop(0, 8, sent, 0)
    for f in range(2):
        for i, which in ((0, 4), (0, 2), (0, 3), (1, 2), (1, 3), (2, 2), (5, 3)):
            copy(f, b, peers[0], i, which).wait_send()

    def tail_copy(stage, r, src, dst, peer):
        return pltpu.make_async_remote_copy(
            src_ref=src, dst_ref=dst,
            send_sem=tail_send.at[stage, r], recv_sem=tail_recv.at[stage, r],
            device_id={"tp": peer}, device_id_type=MESH,
        )

    def columns(c):
        return pl.ds(pl.multiple_of(c * SHARE, SHARE), SHARE)

    def rows_of(q):
        return slice(PIECE * q, PIECE * q + PIECE)

    def chunk_rows(r):
        return slice(ROWS * r, ROWS * r + ROWS)

    def near_copy(stage, q, j):
        at = rows_of(q)
        return tail_copy(
            (0, 2, 7, 8)[2 * j + stage], q, near_out.at[stage, j, at], near_in.at[stage, j, at], twin
        )

    def far_copy(stage, q):
        return tail_copy(
            2 * stage + 1, q, far_out.at[stage, rows_of(q)], far_in.at[stage, rows_of(q)], across
        )

    def give(stage, pieces, j, lhs, w):
        at = slice(PIECE * pieces[0], PIECE * pieces[-1] + PIECE)
        part = jnp.dot(lhs[at, :], w[:, columns((twin + 2 - 2 * j) % 4)], preferred_element_type=jnp.float32)
        near_out[stage, j, at] = part.astype(jnp.bfloat16)
        for q in pieces:
            near_copy(stage, q, j).start()

    def keep(pieces, j, lhs, w):
        at = slice(PIECE * pieces[0], PIECE * pieces[-1] + PIECE)
        kept[j, at] = jnp.dot(lhs[at, :], w[:, columns((across, t)[j])], preferred_element_type=jnp.float32)

    def cross(stage, q):
        at = rows_of(q)
        near_copy(stage, q, 0).wait()
        far_out[stage, at] = (kept[0, at] + near_in[stage, 0, at].astype(jnp.float32)).astype(jnp.bfloat16)
        far_copy(stage, q).start()

    def total(stage, q):
        at = rows_of(q)
        near_copy(stage, q, 1).wait()
        far_copy(stage, q).wait()
        return kept[1, at] + near_in[stage, 1, at].astype(jnp.float32) + far_in[stage, at].astype(jnp.float32)

    def share_copy(stage, q, slot, peer):
        return tail_copy(stage, q, shares.at[q, slot], shares.at[q, slot], peer)

    def chip_rows(chip):
        return pl.ds(pl.multiple_of(chip * 2 * SHARE, 2 * SHARE), 2 * SHARE)

    def norm_part(q, c, add):
        u = shares[q, c].astype(jnp.float32)
        square = jnp.sum(u * u, axis=-1, keepdims=True)
        squares[rows_of(q), :] = squares[rows_of(q), :] + square if add else jnp.broadcast_to(square, (PIECE, 128))
        normed[rows_of(q), columns(c)] = (u * gain2[:, columns(c)]).astype(jnp.bfloat16)

    here = t // 2
    every = range(256 // PIECE)
    loads[4].wait()
    give(0, every, 0, heads, wo)
    keep(every, 0, heads, wo)
    give(0, every, 1, heads, wo)
    for q in every:
        cross(0, q)
    keep(every, 1, heads, wo)

    def share_out(q):
        own = tok[rows_of(q), columns(t)].astype(jnp.float32) + total(0, q)
        resid[rows_of(q), :] = own
        shares[q, t] = own.astype(jnp.bfloat16)
        share_copy(4, q, t, across).start()
        share_copy(5, q, t, twin).start()

    def pieces_of(r):
        return range(ROWS // PIECE * r, ROWS // PIECE * (r + 1))

    def half_units(r):
        for q in pieces_of(r):
            norm_part(q, t, False)
        for q in pieces_of(r):
            share_copy(5, q, twin, twin).wait_recv()
            norm_part(q, twin, True)

        def units(n, _):
            at = pl.ds(pl.multiple_of(n * UNITS, UNITS), UNITS)
            u = normed[chunk_rows(r), chip_rows(here)]
            gated[r, 0, :, at] = jnp.dot(u, wg[chip_rows(here), at], preferred_element_type=jnp.float32)
            gated[r, 1, :, at] = jnp.dot(u, wu[chip_rows(here), at], preferred_element_type=jnp.float32)
            return 0

        lax.fori_loop(0, 2048 // UNITS, units, 0)

    def pass_on(q):
        share_copy(4, q, across, across).wait_recv()
        share_copy(6, q, across, twin).start()

    def other_units(r):
        for q in pieces_of(r):
            norm_part(q, across, True)
        for q in pieces_of(r):
            share_copy(6, q, (twin + 2) % 4, twin).wait_recv()
            norm_part(q, (twin + 2) % 4, True)
        scale = lax.rsqrt(squares[chunk_rows(r), 0:1] * (1.0 / (4 * SHARE)) + EPS)

        def units(n, _):
            at = pl.ds(pl.multiple_of(n * UNITS, UNITS), UNITS)
            u = normed[chunk_rows(r), chip_rows(1 - here)]
            gate = jnp.dot(u, wg[chip_rows(1 - here), at], preferred_element_type=jnp.float32)
            up = jnp.dot(u, wu[chip_rows(1 - here), at], preferred_element_type=jnp.float32)
            gate = (gate + gated[r, 0, :, at]) * scale
            up = (up + gated[r, 1, :, at]) * scale
            hidden[chunk_rows(r), at] = (gate / (1.0 + jnp.exp(-gate)) * up).astype(jnp.bfloat16)
            return 0

        lax.fori_loop(0, 2048 // UNITS, units, 0)

    def down(r):
        pieces = pieces_of(r)
        give(1, pieces, 0, hidden, wd)
        keep(pieces, 0, hidden, wd)
        give(1, pieces, 1, hidden, wd)
        for q in pieces:
            cross(1, q)
        keep(pieces, 1, hidden, wd)

    share_out(0)
    share_out(1)
    loads[5].wait()
    loads[6].wait()
    half_units(0)
    share_out(2)
    share_out(3)
    pass_on(0)
    half_units(1)
    pass_on(1)
    loads[7].wait()
    other_units(0)
    pass_on(2)
    pass_on(3)
    down(0)
    other_units(1)
    down(1)
    for q in every:
        out[rows_of(q), :] = (resid[rows_of(q), :] + total(1, q)).astype(jnp.bfloat16)
    for q in every:
        share_copy(4, q, t, across).wait_send()
        share_copy(5, q, t, twin).wait_send()
        share_copy(6, q, across, twin).wait_send()


def layer(tok, order, gain, wq, wk, wv, tab, gain2, wo, wg, wu, wd):
    vmem = pl.BlockSpec(memory_space=pltpu.VMEM)
    hbm = pl.BlockSpec(memory_space=pl.ANY)
    bf16, f32 = jnp.bfloat16, jnp.float32
    return pl.pallas_call(
        layer_kernel,
        out_shape=jax.ShapeDtypeStruct((256, SHARE), bf16),
        in_specs=[hbm, pl.BlockSpec(memory_space=pltpu.SMEM), vmem, hbm, hbm, hbm, vmem, vmem, hbm, hbm, hbm, hbm],
        out_specs=vmem,
        scratch_shapes=[
            pltpu.VMEM((256, 256), f32),
            pltpu.VMEM((8, 256), jnp.int32),
            pltpu.VMEM((CHUNKS, 2, ROWS, 2048), f32),
            pltpu.VMEM((256, 128), f32),
            pltpu.VMEM((256, 2048), bf16),
            pltpu.VMEM((2048, 512), bf16),
            pltpu.VMEM((2048, 128), bf16),
            pltpu.VMEM((2048, 128), bf16),
            pltpu.VMEM((512, 2048), bf16),
            pltpu.VMEM((2048, 2048), bf16),
            pltpu.VMEM((2048, 2048), bf16),
            pltpu.VMEM((2048, 2048), bf16),
            pltpu.VMEM((256, 512), bf16),
            pltpu.VMEM((2, 2, 256, SHARE), bf16),
            pltpu.VMEM((2, 2, 256, SHARE), bf16),
            pltpu.VMEM((2, 256, SHARE), bf16),
            pltpu.VMEM((2, 256, SHARE), bf16),
            pltpu.VMEM((2, 256, SHARE), f32),
            pltpu.VMEM((256, SHARE), f32),
            pltpu.VMEM((256 // PIECE, 4, PIECE, SHARE), bf16),
            pltpu.VMEM((256, 2048), bf16),
            pltpu.SemaphoreType.DMA((8,)),
            pltpu.SemaphoreType.DMA((9, 256 // PIECE)),
            pltpu.SemaphoreType.DMA((9, 256 // PIECE)),
            pltpu.VMEM((256, 2048), bf16),
            pltpu.VMEM((64, 256, 128), bf16),
            pltpu.VMEM((2, 4, 128, 256), bf16),
            pltpu.VMEM((8, 256, 256), f32),
            pltpu.VMEM((2, 8, 256), f32),
            pltpu.VMEM((8, 256), f32),
            pltpu.VMEM((8, 256), f32),
            pltpu.VMEM((8, 256), f32),
            pltpu.VMEM((512, 256), f32),
            pltpu.SemaphoreType.DMA((2, 8, 6)),
            pltpu.SemaphoreType.DMA((64,)),
        ],
        compiler_params=pltpu.CompilerParams(
            collective_id=0, has_side_effects=True, vmem_limit_bytes=62 * 1024 * 1024
        ),
        name="layer",
    )(tok, order, gain, wq, wk, wv, tab, gain2, wo, wg, wu, wd)


def local(tokens, order, gain_attn, gain_ffn, w_query, w_key, w_value, w_out, w_gate, w_up, w_down):
    return layer(
        tokens, order, gain_attn[None, :], w_query, w_key, w_value, jnp.asarray(rope_table()),
        gain_ffn[None, :], w_out, w_gate, w_up, w_down,
    )


def solution(mesh):
    placed = (
        P("blk", None),
        P(),
        P(),
        P(),
        P(None, "tp"),
        P(None, "tp"),
        P(None, "tp"),
        P("tp", None),
        P(None, "tp"),
        P(None, "tp"),
        P("tp", None),
    )
    return jax.shard_map(
        local, mesh=mesh, in_specs=placed, out_specs=P("blk", "tp"), check_vma=False
    )
```

```python
import jax
import jax.numpy as jnp
import numpy as np
from jax import lax
from jax.experimental import pallas as pl
from jax.experimental.pallas import tpu as pltpu
from jax.sharding import PartitionSpec as P

HD = 64
SHARE = 512
CHUNKS = 2
ROWS = 256 // CHUNKS
PIECE = 64
UNITS = 512
EPS = 1e-05
ROPE_BASE = 500000.0
BIG = 1e30
LOG2E = 1.4426950408889634
MESH = pl.DeviceIdType.MESH


ORDER = (
    (2, 0), (4, 0), (0, 3), (0, 1), (1, 0), (2, 1), (6, 0), (2, 3),
    (4, 1), (4, 3), (5, 0), (1, 3), (0, 2), (6, 1), (2, 2), (3, 0),
    (1, 1), (6, 3), (7, 0), (5, 3), (5, 1), (3, 1), (4, 2), (6, 2),
    (1, 2), (7, 1), (3, 3), (7, 3), (3, 2), (5, 2), (7, 2),
)
EVENTS = (
    ((2, 0), (4, 0)),
    (),
    ((0, 3), (0, 1)),
    (),
    ((1, 0),),
    ((6, 0), (2, 1)),
    (),
    ((2, 3), (4, 1)),
    (),
    ((5, 0), (4, 3)),
    (),
    ((1, 3),),
    ((6, 1), (0, 2)),
    (),
    ((3, 0), (2, 2)),
    (),
    ((1, 1),),
    ((7, 0), (6, 3)),
    (),
    ((5, 3), (5, 1)),
    (),
    ((3, 1),),
    ((4, 2), (6, 2)),
    (),
    ((1, 2), (7, 1)),
    (),
    ((3, 3),),
    ((7, 3),),
    ((3, 2),),
    ((5, 2),),
    ((7, 2),),
    (),
)
CODES = [sum((4 * i + ds) << (5 * j) for j, (i, ds) in enumerate(ORDER[p : p + 6])) for p in range(0, 31, 6)]


def rope_table():
    freq = ROPE_BASE ** (-np.arange(HD // 2) * 2.0 / HD)[:, None]
    within = freq * np.arange(128)[None, :]
    starts = freq * (128.0 * np.arange(128))[None, :]
    return np.concatenate([np.cos(within), np.sin(within), np.cos(starts), np.sin(starts)]).astype(np.float32)


def origin(flow, major, minor, x):
    if flow == 0:
        return minor * 8 + major * 2 + x
    return major * 8 + minor * 2 + x


def plane(i, major, x):
    k = i // 2
    step = (3 * k + 3 * (k // 2) + 2 * (k // 3)) % 4
    return (major + step) % 4, (x + i) % 2


def layer_kernel(
    tok_hbm, order, gain, wq_hbm, wk_hbm, wv_hbm, tab, gain2, wo_hbm, wg_hbm, wu_hbm, wd_hbm,
    out, diag, blocks, gated, squares, tok, wq, wk, wv, wo, wg, wu, wd, heads, near_out, near_in, far_out, far_in, kept, resid,
    shares, hidden, load_sem, tail_send, tail_recv, normed, kv, qp, s_ref, mo_ref, f_ref, m_ref, l_ref, acc, send_sem, recv_sem,
):
    b = lax.axis_index("blk")
    z, y, x = b // 8, (b // 2) % 4, b % 2
    coords = ((y, z), (z, y))

    t = lax.axis_index("tp")
    core = t % 2
    twin = t + 1 - 2 * core
    across = (t + 2) % 4
    loads = [
        pltpu.make_async_copy(src, dst, load_sem.at[i])
        for i, (src, dst) in enumerate(
            ((tok_hbm, tok), (wk_hbm, wk), (wv_hbm, wv), (wq_hbm, wq))
            + ((wo_hbm, wo), (wg_hbm, wg), (wu_hbm, wu), (wd_hbm, wd))
        )
    ]
    for load in loads[:4]:
        load.start()
    barrier = pltpu.get_barrier_semaphore()
    for peer in (twin, across):
        pl.semaphore_signal(barrier, inc=1, device_id={"tp": peer}, device_id_type=MESH)
    peers = [origin(0, y, z, (x + 1) % 2)]
    peers += [origin(0, (y + d) % 4, z, x) for d in (1, 3)]
    peers += [origin(0, y, (z + d) % 4, x) for d in (1, 3)]
    for peer in peers:
        pl.semaphore_signal(barrier, inc=1, device_id={"blk": peer}, device_id_type=MESH)

    rows = 64
    loads[0].wait()

    def norm_rows(r, _):
        at = pl.ds(pl.multiple_of(r * rows, rows), rows)
        t = tok[at, :].astype(jnp.float32)
        scale = lax.rsqrt(jnp.mean(t * t, axis=-1, keepdims=True) + EPS)
        normed[at, :] = (t * scale * gain[...]).astype(jnp.bfloat16)
        return 0

    lax.fori_loop(0, 256 // rows, norm_rows, 0)

    first, second = order[2 * b], order[2 * b + 1]
    lane = lax.broadcasted_iota(jnp.int32, (32, 128), 1)
    cosines, sines = [], []
    for block in (first, second):
        ca = jnp.sum(jnp.where(lane == block, tab[64:96, :], 0.0), axis=1, keepdims=True)
        sa = jnp.sum(jnp.where(lane == block, tab[96:128, :], 0.0), axis=1, keepdims=True)
        cosines.append(ca * tab[0:32, :] - sa * tab[32:64, :])
        sines.append(sa * tab[0:32, :] + ca * tab[32:64, :])
    c = jnp.concatenate(cosines, axis=1)
    s = jnp.concatenate(sines, axis=1)

    def rotated(u):
        a, h = u[0:32], u[32:64]
        return jnp.concatenate([a * c - h * s, h * c + a * s], axis=0)

    loads[1].wait()
    loads[2].wait()
    k = jnp.dot(normed[...], wk[...], preferred_element_type=jnp.float32).T
    kt = jnp.concatenate([rotated(k[0:64]), rotated(k[64:128])], axis=0)
    kn = kt.T.astype(jnp.bfloat16)
    v = jnp.dot(normed[...], wv[...], preferred_element_type=jnp.float32).T.astype(jnp.bfloat16)
    for f in range(2):
        kv[2 * b + f, 0:128, :] = kn[128 * f : 128 * f + 128, :]
        kv[2 * b + f, 128:256, :] = v[:, 128 * f : 128 * f + 128]

    pl.semaphore_wait(barrier, 7)

    def copy(f, org, dest, i, which):
        unit = 2 * org + f
        return pltpu.make_async_remote_copy(
            src_ref=kv.at[unit], dst_ref=kv.at[unit],
            send_sem=send_sem.at[f, i, which], recv_sem=recv_sem.at[unit],
            device_id={"blk": dest}, device_id_type=MESH,
        )

    def arrived(f, org):
        unit = 2 * org + f
        pltpu.make_async_remote_copy(
            src_ref=kv.at[unit], dst_ref=kv.at[unit],
            send_sem=send_sem.at[f, 0, 0], recv_sem=recv_sem.at[unit],
            device_id={"blk": peers[0]}, device_id_type=MESH,
        ).wait_recv()

    for f in range(2):
        major, minor = coords[f]
        copy(f, b, origin(f, major, minor, (x + 1) % 2), 0, 4).start()
    for f in range(2):
        major, minor = coords[f]
        copy(f, b, origin(f, (major + 1) % 4, minor, x), 0, 2).start()
        copy(f, b, origin(f, (major + 3) % 4, minor, x), 0, 3).start()
    for f in range(2):
        major, minor = coords[f]
        copy(f, b, origin(f, major, (minor + 1) % 4, x), 0, 0).start()
        copy(f, b, origin(f, major, (minor + 3) % 4, x), 0, 1).start()

    column = lax.broadcasted_iota(jnp.int32, (8, 256), 1)
    block_row = jnp.where(column < 128, first, second)
    blocks[...] = block_row
    place = block_row[0:1] * 128 + column[0:1] % 128
    for f, block in enumerate((first, second)):
        key_place = block * 128 + lax.broadcasted_iota(jnp.int32, (128, 256), 0)
        diag[128 * f : 128 * f + 128, :] = jnp.where(key_place <= place, 0.0, -BIG)

    loads[3].wait()
    for load in loads[4:]:
        load.start()
    zero = jnp.zeros((64, 256), jnp.bfloat16)
    for half in range(2):
        q = jnp.dot(
            normed[...], wq[:, 256 * half : 256 * half + 256], preferred_element_type=jnp.float32
        ).T
        for n in range(4):
            u = (rotated(q[64 * n : 64 * n + 64]) * (HD**-0.5 * LOG2E)).astype(jnp.bfloat16)
            top, low = (u, zero) if half == 0 else (zero, u)
            qp[half, n, 0:64, :] = top
            qp[half, n, 64:128, :] = low

    def weigh(row, ja, jb, first):
        g, n = row // 4, row % 4
        pa = jnp.exp2(s_ref[row, 0:128, :] - mo_ref[0, row : row + 1, :])
        pb = jnp.exp2(s_ref[row, 128:256, :] - mo_ref[1, row : row + 1, :])
        p = jnp.concatenate([pa, pb], axis=0).astype(jnp.bfloat16)
        va = kv[ja, 128 + 64 * g : 192 + 64 * g, :]
        vb = kv[jb, 128 + 64 * g : 192 + 64 * g, :]
        vt = jnp.concatenate([jnp.concatenate([va, vb], axis=1), jnp.ones((16, 256), jnp.bfloat16)], axis=0)
        o = jnp.dot(vt, p, preferred_element_type=jnp.float32)
        total, o = o[64:65], o[0:64]
        if first:
            l_ref[row : row + 1, :] = total
            acc[64 * row : 64 * row + 64, :] = o
        else:
            factor = f_ref[row : row + 1, :]
            l_ref[row : row + 1, :] = l_ref[row : row + 1, :] * factor + total
            acc[64 * row : 64 * row + 64, :] = acc[64 * row : 64 * row + 64, :] * factor + o

    def score(row, ja, jb, first):
        g, n = row // 4, row % 4
        sa = jnp.dot(kv[ja, 0:128, :], qp[g, n], preferred_element_type=jnp.float32)
        sb = jnp.dot(kv[jb, 0:128, :], qp[g, n], preferred_element_type=jnp.float32)
        if first:
            sa = sa + diag[0:128, :]
            sb = sb + diag[128:256, :]
        s_ref[row, 0:128, :] = sa
        s_ref[row, 128:256, :] = sb
        ma, mb = jnp.max(sa, axis=0, keepdims=True), jnp.max(sb, axis=0, keepdims=True)
        if first:
            new = jnp.maximum(ma, mb)
            mo_ref[0, row : row + 1, :] = new
            mo_ref[1, row : row + 1, :] = new
        else:
            ba = jnp.where(blocks[0:1, :] < order[ja], BIG, 0.0)
            bb = jnp.where(blocks[0:1, :] < order[jb], BIG, 0.0)
            old = m_ref[row : row + 1, :]
            new = jnp.maximum(old, jnp.maximum(ma - ba, mb - bb))
            f_ref[row : row + 1, :] = jnp.exp2(old - new)
            mo_ref[0, row : row + 1, :] = new + ba
            mo_ref[1, row : row + 1, :] = new + bb
        m_ref[row : row + 1, :] = new

    def attend(before, now):
        for row in range(8):
            weigh(row, *before, False)
            score(row, *now, False)
        return now

    for row in range(8):
        score(row, 2 * b, 2 * b + 1, True)
    for row in range(8):
        l_ref[row : row + 1, :] = jnp.zeros((1, 256), jnp.float32)
        acc[64 * row : 64 * row + 64, :] = jnp.zeros((64, 256), jnp.float32)
        f_ref[row : row + 1, :] = jnp.zeros((1, 256), jnp.float32)
    held = (2 * b, 2 * b + 1)

    def source(f, i, ds):
        major, minor = coords[f]
        pp, xx = plane(i, major, x)
        return origin(f, pp, (minor + ds) % 4, xx)

    def take(i, ds):
        for f in range(2):
            major, minor = coords[f]
            org = source(f, i, ds)
            arrived(f, org)
            if ds == 0:
                if i in (1, 2):
                    copy(f, org, origin(f, (major + 1) % 4, minor, x), i, 2).start()
                if i in (1, 5):
                    copy(f, org, origin(f, (major + 3) % 4, minor, x), i, 3).start()
                if i not in (1, 3):
                    copy(f, org, origin(f, major, (minor + 1) % 4, x), i, 0).start()
                    copy(f, org, origin(f, major, (minor + 3) % 4, x), i, 1).start()
            elif ds != 2:
                if i in (0, 2):
                    copy(f, org, origin(f, major, minor, (x + 1) % 2), i + 1, ds // 3).start()
                if (i // 2) % 2 == (ds == 1):
                    copy(f, org, origin(f, major, (minor + 4 - ds) % 4, x), i, 5).start()

    def one_step(n, held):
        for group in range(0, 32, 8):

            @pl.when(n // 8 == group // 8)
            def _():
                for at in range(group, group + 8):
                    if EVENTS[at]:

                        @pl.when(n == at)
                        def _():
                            for i, ds in EVENTS[at]:
                                take(i, ds)

        code = jnp.int32(CODES[-1])
        for part in range(len(CODES) - 2, -1, -1):
            code = jnp.where(n < 6 * part + 6, CODES[part], code)
        code = lax.shift_right_logical(code, 5 * (n % 6)) % 32
        i, ds = code // 4, code % 4
        return attend(held, (2 * source(0, i, ds), 2 * source(1, i, ds) + 1))

    held = lax.fori_loop(0, 31, one_step, held)
    for row in range(8):
        weigh(row, *held, False)

    for n in range(8):
        inv = 1.0 / l_ref[n : n + 1, :]
        heads[:, 64 * n : 64 * n + 64] = (acc[64 * n : 64 * n + 64, :] * inv).T.astype(jnp.bfloat16)

    def sent(i, _):
        for f in range(2):
            for which in (0, 1, 5):
                copy(f, b, peers[0], i, which).wait_send()
        return 0

    lax.fori_loop(0, 8, sent, 0)
    for f in range(2):
        for i, which in ((0, 4), (0, 2), (0, 3), (1, 2), (1, 3), (2, 2), (5, 3)):
            copy(f, b, peers[0], i, which).wait_send()

    def tail_copy(stage, r, src, dst, peer):
        return pltpu.make_async_remote_copy(
            src_ref=src, dst_ref=dst,
            send_sem=tail_send.at[stage, r], recv_sem=tail_recv.at[stage, r],
            device_id={"tp": peer}, device_id_type=MESH,
        )

    def columns(c):
        return pl.ds(pl.multiple_of(c * SHARE, SHARE), SHARE)

    def rows_of(q):
        return slice(PIECE * q, PIECE * q + PIECE)

    def chunk_rows(r):
        return slice(ROWS * r, ROWS * r + ROWS)

    def near_copy(stage, q, j):
        at = rows_of(q)
        return tail_copy(
            (0, 2, 7, 8)[2 * j + stage], q, near_out.at[stage, j, at], near_in.at[stage, j, at], twin
        )

    def far_copy(stage, q):
        return tail_copy(
            2 * stage + 1, q, far_out.at[stage, rows_of(q)], far_in.at[stage, rows_of(q)], across
        )

    def give(stage, pieces, j, lhs, w):
        at = slice(PIECE * pieces[0], PIECE * pieces[-1] + PIECE)
        part = jnp.dot(lhs[at, :], w[:, columns((twin + 2 - 2 * j) % 4)], preferred_element_type=jnp.float32)
        near_out[stage, j, at] = part.astype(jnp.bfloat16)
        for q in pieces:
            near_copy(stage, q, j).start()

    def keep(pieces, j, lhs, w):
        at = slice(PIECE * pieces[0], PIECE * pieces[-1] + PIECE)
        kept[j, at] = jnp.dot(lhs[at, :], w[:, columns((across, t)[j])], preferred_element_type=jnp.float32)

    def cross(stage, q):
        at = rows_of(q)
        near_copy(stage, q, 0).wait()
        far_out[stage, at] = (kept[0, at] + near_in[stage, 0, at].astype(jnp.float32)).astype(jnp.bfloat16)
        far_copy(stage, q).start()

    def total(stage, q):
        at = rows_of(q)
        near_copy(stage, q, 1).wait()
        far_copy(stage, q).wait()
        return kept[1, at] + near_in[stage, 1, at].astype(jnp.float32) + far_in[stage, at].astype(jnp.float32)

    def share_copy(stage, q, slot, peer):
        return tail_copy(stage, q, shares.at[q, slot], shares.at[q, slot], peer)

    def chip_rows(chip):
        return pl.ds(pl.multiple_of(chip * 2 * SHARE, 2 * SHARE), 2 * SHARE)

    def norm_part(q, c, add):
        u = shares[q, c].astype(jnp.float32)
        square = jnp.sum(u * u, axis=-1, keepdims=True)
        squares[rows_of(q), :] = squares[rows_of(q), :] + square if add else jnp.broadcast_to(square, (PIECE, 128))
        normed[rows_of(q), columns(c)] = (u * gain2[:, columns(c)]).astype(jnp.bfloat16)

    here = t // 2
    every = range(256 // PIECE)
    loads[4].wait()
    give(0, every, 0, heads, wo)
    keep(every, 0, heads, wo)
    give(0, every, 1, heads, wo)
    for q in every:
        cross(0, q)
    keep(every, 1, heads, wo)

    def share_out(q):
        own = tok[rows_of(q), columns(t)].astype(jnp.float32) + total(0, q)
        resid[rows_of(q), :] = own
        shares[q, t] = own.astype(jnp.bfloat16)
        share_copy(4, q, t, across).start()
        share_copy(5, q, t, twin).start()

    def pieces_of(r):
        return range(ROWS // PIECE * r, ROWS // PIECE * (r + 1))

    def half_units(r):
        for q in pieces_of(r):
            norm_part(q, t, False)
        for q in pieces_of(r):
            share_copy(5, q, twin, twin).wait_recv()
            norm_part(q, twin, True)

        def units(n, _):
            at = pl.ds(pl.multiple_of(n * UNITS, UNITS), UNITS)
            u = normed[chunk_rows(r), chip_rows(here)]
            gated[r, 0, :, at] = jnp.dot(u, wg[chip_rows(here), at], preferred_element_type=jnp.float32)
            gated[r, 1, :, at] = jnp.dot(u, wu[chip_rows(here), at], preferred_element_type=jnp.float32)
            return 0

        lax.fori_loop(0, 2048 // UNITS, units, 0)

    def pass_on(q):
        share_copy(4, q, across, across).wait_recv()
        share_copy(6, q, across, twin).start()

    def other_units(r):
        for q in pieces_of(r):
            norm_part(q, across, True)
        for q in pieces_of(r):
            share_copy(6, q, (twin + 2) % 4, twin).wait_recv()
            norm_part(q, (twin + 2) % 4, True)
        scale = lax.rsqrt(squares[chunk_rows(r), 0:1] * (1.0 / (4 * SHARE)) + EPS)

        def units(n, _):
            at = pl.ds(pl.multiple_of(n * UNITS, UNITS), UNITS)
            u = normed[chunk_rows(r), chip_rows(1 - here)]
            gate = jnp.dot(u, wg[chip_rows(1 - here), at], preferred_element_type=jnp.float32)
            up = jnp.dot(u, wu[chip_rows(1 - here), at], preferred_element_type=jnp.float32)
            gate = (gate + gated[r, 0, :, at]) * scale
            up = (up + gated[r, 1, :, at]) * scale
            hidden[chunk_rows(r), at] = (gate / (1.0 + jnp.exp(-gate)) * up).astype(jnp.bfloat16)
            return 0

        lax.fori_loop(0, 2048 // UNITS, units, 0)

    def down(r):
        pieces = pieces_of(r)
        give(1, pieces, 0, hidden, wd)
        keep(pieces, 0, hidden, wd)
        give(1, pieces, 1, hidden, wd)
        for q in pieces:
            cross(1, q)
        keep(pieces, 1, hidden, wd)

    share_out(0)
    share_out(1)
    loads[5].wait()
    loads[6].wait()
    half_units(0)
    share_out(2)
    share_out(3)
    pass_on(0)
    half_units(1)
    pass_on(1)
    loads[7].wait()
    other_units(0)
    pass_on(2)
    pass_on(3)
    down(0)
    other_units(1)
    down(1)
    for q in every:
        out[rows_of(q), :] = (resid[rows_of(q), :] + total(1, q)).astype(jnp.bfloat16)
    for q in every:
        share_copy(4, q, t, across).wait_send()
        share_copy(5, q, t, twin).wait_send()
        share_copy(6, q, across, twin).wait_send()


def layer(tok, order, gain, wq, wk, wv, tab, gain2, wo, wg, wu, wd):
    vmem = pl.BlockSpec(memory_space=pltpu.VMEM)
    hbm = pl.BlockSpec(memory_space=pl.ANY)
    bf16, f32 = jnp.bfloat16, jnp.float32
    return pl.pallas_call(
        layer_kernel,
        out_shape=jax.ShapeDtypeStruct((256, SHARE), bf16),
        in_specs=[hbm, pl.BlockSpec(memory_space=pltpu.SMEM), vmem, hbm, hbm, hbm, vmem, vmem, hbm, hbm, hbm, hbm],
        out_specs=vmem,
        scratch_shapes=[
            pltpu.VMEM((256, 256), f32),
            pltpu.VMEM((8, 256), jnp.int32),
            pltpu.VMEM((CHUNKS, 2, ROWS, 2048), f32),
            pltpu.VMEM((256, 128), f32),
            pltpu.VMEM((256, 2048), bf16),
            pltpu.VMEM((2048, 512), bf16),
            pltpu.VMEM((2048, 128), bf16),
            pltpu.VMEM((2048, 128), bf16),
            pltpu.VMEM((512, 2048), bf16),
            pltpu.VMEM((2048, 2048), bf16),
            pltpu.VMEM((2048, 2048), bf16),
            pltpu.VMEM((2048, 2048), bf16),
            pltpu.VMEM((256, 512), bf16),
            pltpu.VMEM((2, 2, 256, SHARE), bf16),
            pltpu.VMEM((2, 2, 256, SHARE), bf16),
            pltpu.VMEM((2, 256, SHARE), bf16),
            pltpu.VMEM((2, 256, SHARE), bf16),
            pltpu.VMEM((2, 256, SHARE), f32),
            pltpu.VMEM((256, SHARE), f32),
            pltpu.VMEM((256 // PIECE, 4, PIECE, SHARE), bf16),
            pltpu.VMEM((256, 2048), bf16),
            pltpu.SemaphoreType.DMA((8,)),
            pltpu.SemaphoreType.DMA((9, 256 // PIECE)),
            pltpu.SemaphoreType.DMA((9, 256 // PIECE)),
            pltpu.VMEM((256, 2048), bf16),
            pltpu.VMEM((64, 256, 128), bf16),
            pltpu.VMEM((2, 4, 128, 256), bf16),
            pltpu.VMEM((8, 256, 256), f32),
            pltpu.VMEM((2, 8, 256), f32),
            pltpu.VMEM((8, 256), f32),
            pltpu.VMEM((8, 256), f32),
            pltpu.VMEM((8, 256), f32),
            pltpu.VMEM((512, 256), f32),
            pltpu.SemaphoreType.DMA((2, 8, 6)),
            pltpu.SemaphoreType.DMA((64,)),
        ],
        compiler_params=pltpu.CompilerParams(
            collective_id=0, has_side_effects=True, vmem_limit_bytes=62 * 1024 * 1024
        ),
        name="layer",
    )(tok, order, gain, wq, wk, wv, tab, gain2, wo, wg, wu, wd)


def local(tokens, order, gain_attn, gain_ffn, w_query, w_key, w_value, w_out, w_gate, w_up, w_down):
    return layer(
        tokens, order, gain_attn[None, :], w_query, w_key, w_value, jnp.asarray(rope_table()),
        gain_ffn[None, :], w_out, w_gate, w_up, w_down,
    )


def solution(mesh):
    placed = (
        P("blk", None),
        P(),
        P(),
        P(),
        P(None, "tp"),
        P(None, "tp"),
        P(None, "tp"),
        P("tp", None),
        P(None, "tp"),
        P(None, "tp"),
        P("tp", None),
    )
    return jax.shard_map(
        local, mesh=mesh, in_specs=placed, out_specs=P("blk", "tp"), check_vma=False
    )
```

```python
import jax
import jax.numpy as jnp
import numpy as np
from jax import lax
from jax.experimental import pallas as pl
from jax.experimental.pallas import tpu as pltpu
from jax.sharding import PartitionSpec as P

HD = 64
SHARE = 512
CHUNKS = 2
ROWS = 256 // CHUNKS
PIECE = 64
UNITS = 512
EPS = 1e-05
ROPE_BASE = 500000.0
BIG = 1e30
LOG2E = 1.4426950408889634
MESH = pl.DeviceIdType.MESH


ORDER = (
    (2, 0), (4, 0), (0, 3), (0, 1), (1, 0), (2, 1), (6, 0), (2, 3),
    (4, 1), (4, 3), (5, 0), (1, 3), (0, 2), (6, 1), (2, 2), (3, 0),
    (1, 1), (6, 3), (7, 0), (5, 3), (5, 1), (3, 1), (4, 2), (6, 2),
    (1, 2), (7, 1), (3, 3), (7, 3), (3, 2), (5, 2), (7, 2),
)
EVENTS = (
    ((2, 0), (4, 0)),
    (),
    ((0, 3), (0, 1)),
    (),
    ((1, 0),),
    ((6, 0), (2, 1)),
    (),
    ((2, 3), (4, 1)),
    (),
    ((5, 0), (4, 3)),
    (),
    ((1, 3),),
    ((6, 1), (0, 2)),
    (),
    ((3, 0), (2, 2)),
    (),
    ((1, 1),),
    ((7, 0), (6, 3)),
    (),
    ((5, 3), (5, 1)),
    (),
    ((3, 1),),
    ((4, 2), (6, 2)),
    (),
    ((1, 2), (7, 1)),
    (),
    ((3, 3),),
    ((7, 3),),
    ((3, 2),),
    ((5, 2),),
    ((7, 2),),
    (),
)
CODES = [sum((4 * i + ds) << (5 * j) for j, (i, ds) in enumerate(ORDER[p : p + 6])) for p in range(0, 31, 6)]


def rope_table():
    freq = ROPE_BASE ** (-np.arange(HD // 2) * 2.0 / HD)[:, None]
    within = freq * np.arange(128)[None, :]
    starts = freq * (128.0 * np.arange(128))[None, :]
    return np.concatenate([np.cos(within), np.sin(within), np.cos(starts), np.sin(starts)]).astype(np.float32)


def origin(flow, major, minor, x):
    if flow == 0:
        return minor * 8 + major * 2 + x
    return major * 8 + minor * 2 + x


def plane(i, major, x):
    k = i // 2
    step = (3 * k + 3 * (k // 2) + 2 * (k // 3)) % 4
    return (major + step) % 4, (x + i) % 2


def layer_kernel(
    tok_hbm, order, gain, wq_hbm, wk_hbm, wv_hbm, tab, gain2, wo_hbm, wg_hbm, wu_hbm, wd_hbm,
    out, diag, blocks, gated, squares, tok, wq, wk, wv, wo, wg, wu, wd, heads, near_out, near_in, far_out, far_in, kept, resid,
    shares, hidden, load_sem, tail_send, tail_recv, normed, kv, qp, s_ref, mo_ref, f_ref, m_ref, l_ref, acc, send_sem, recv_sem,
):
    b = lax.axis_index("blk")
    z, y, x = b // 8, (b // 2) % 4, b % 2
    coords = ((y, z), (z, y))

    t = lax.axis_index("tp")
    core = t % 2
    twin = t + 1 - 2 * core
    across = (t + 2) % 4
    loads = [
        pltpu.make_async_copy(src, dst, load_sem.at[i])
        for i, (src, dst) in enumerate(
            ((tok_hbm.at[0:64], tok.at[0:64]), (wk_hbm, wk), (wv_hbm, wv), (wq_hbm, wq))
            + ((wo_hbm, wo), (wg_hbm, wg), (wu_hbm, wu), (wd_hbm, wd))
        )
    ]
    more = [
        pltpu.make_async_copy(
            tok_hbm.at[64 * r : 64 * r + 64], tok.at[64 * r : 64 * r + 64], load_sem.at[7 + r]
        )
        for r in range(1, 4)
    ]
    for load in (loads[0], *more, *loads[1:4]):
        load.start()
    barrier = pltpu.get_barrier_semaphore()
    for peer in (twin, across):
        pl.semaphore_signal(barrier, inc=1, device_id={"tp": peer}, device_id_type=MESH)
    peers = [origin(0, y, z, (x + 1) % 2)]
    peers += [origin(0, (y + d) % 4, z, x) for d in (1, 3)]
    peers += [origin(0, y, (z + d) % 4, x) for d in (1, 3)]
    for peer in peers:
        pl.semaphore_signal(barrier, inc=1, device_id={"blk": peer}, device_id_type=MESH)

    for r, load in enumerate((loads[0], *more)):
        load.wait()
        at = slice(64 * r, 64 * r + 64)
        wide = tok[at, :].astype(jnp.float32)
        scale = lax.rsqrt(jnp.mean(wide * wide, axis=-1, keepdims=True) + EPS)
        normed[at, :] = (wide * scale * gain[...]).astype(jnp.bfloat16)

    first, second = order[2 * b], order[2 * b + 1]
    lane = lax.broadcasted_iota(jnp.int32, (32, 128), 1)
    cosines, sines = [], []
    for block in (first, second):
        ca = jnp.sum(jnp.where(lane == block, tab[64:96, :], 0.0), axis=1, keepdims=True)
        sa = jnp.sum(jnp.where(lane == block, tab[96:128, :], 0.0), axis=1, keepdims=True)
        cosines.append(ca * tab[0:32, :] - sa * tab[32:64, :])
        sines.append(sa * tab[0:32, :] + ca * tab[32:64, :])
    c = jnp.concatenate(cosines, axis=1)
    s = jnp.concatenate(sines, axis=1)

    def rotated(u):
        a, h = u[0:32], u[32:64]
        return jnp.concatenate([a * c - h * s, h * c + a * s], axis=0)

    loads[1].wait()
    loads[2].wait()
    k = jnp.dot(normed[...], wk[...], preferred_element_type=jnp.float32).T
    kt = jnp.concatenate([rotated(k[0:64]), rotated(k[64:128])], axis=0)
    kn = kt.T.astype(jnp.bfloat16)
    v = jnp.dot(normed[...], wv[...], preferred_element_type=jnp.float32).T.astype(jnp.bfloat16)
    for f in range(2):
        kv[2 * b + f, 0:128, :] = kn[128 * f : 128 * f + 128, :]
        kv[2 * b + f, 128:256, :] = v[:, 128 * f : 128 * f + 128]

    pl.semaphore_wait(barrier, 7)

    def copy(f, org, dest, i, which):
        unit = 2 * org + f
        return pltpu.make_async_remote_copy(
            src_ref=kv.at[unit], dst_ref=kv.at[unit],
            send_sem=send_sem.at[f, i, which], recv_sem=recv_sem.at[unit],
            device_id={"blk": dest}, device_id_type=MESH,
        )

    def arrived(f, org):
        unit = 2 * org + f
        pltpu.make_async_remote_copy(
            src_ref=kv.at[unit], dst_ref=kv.at[unit],
            send_sem=send_sem.at[f, 0, 0], recv_sem=recv_sem.at[unit],
            device_id={"blk": peers[0]}, device_id_type=MESH,
        ).wait_recv()

    for f in range(2):
        major, minor = coords[f]
        copy(f, b, origin(f, major, minor, (x + 1) % 2), 0, 4).start()
    for f in range(2):
        major, minor = coords[f]
        copy(f, b, origin(f, (major + 1) % 4, minor, x), 0, 2).start()
        copy(f, b, origin(f, (major + 3) % 4, minor, x), 0, 3).start()
    for f in range(2):
        major, minor = coords[f]
        copy(f, b, origin(f, major, (minor + 1) % 4, x), 0, 0).start()
        copy(f, b, origin(f, major, (minor + 3) % 4, x), 0, 1).start()

    column = lax.broadcasted_iota(jnp.int32, (8, 256), 1)
    block_row = jnp.where(column < 128, first, second)
    blocks[...] = block_row
    place = block_row[0:1] * 128 + column[0:1] % 128
    for f, block in enumerate((first, second)):
        key_place = block * 128 + lax.broadcasted_iota(jnp.int32, (128, 256), 0)
        diag[128 * f : 128 * f + 128, :] = jnp.where(key_place <= place, 0.0, -BIG)

    loads[3].wait()
    for load in loads[4:]:
        load.start()
    zero = jnp.zeros((64, 256), jnp.bfloat16)
    for half in range(2):
        q = jnp.dot(
            normed[...], wq[:, 256 * half : 256 * half + 256], preferred_element_type=jnp.float32
        ).T
        for n in range(4):
            u = (rotated(q[64 * n : 64 * n + 64]) * (HD**-0.5 * LOG2E)).astype(jnp.bfloat16)
            top, low = (u, zero) if half == 0 else (zero, u)
            qp[half, n, 0:64, :] = top
            qp[half, n, 64:128, :] = low

    def weigh(row, ja, jb, first):
        g, n = row // 4, row % 4
        pa = jnp.exp2(s_ref[row, 0:128, :] - mo_ref[0, row : row + 1, :])
        pb = jnp.exp2(s_ref[row, 128:256, :] - mo_ref[1, row : row + 1, :])
        p = jnp.concatenate([pa, pb], axis=0).astype(jnp.bfloat16)
        va = kv[ja, 128 + 64 * g : 192 + 64 * g, :]
        vb = kv[jb, 128 + 64 * g : 192 + 64 * g, :]
        vt = jnp.concatenate([jnp.concatenate([va, vb], axis=1), jnp.ones((16, 256), jnp.bfloat16)], axis=0)
        o = jnp.dot(vt, p, preferred_element_type=jnp.float32)
        total, o = o[64:65], o[0:64]
        if first:
            l_ref[row : row + 1, :] = total
            acc[64 * row : 64 * row + 64, :] = o
        else:
            factor = f_ref[row : row + 1, :]
            l_ref[row : row + 1, :] = l_ref[row : row + 1, :] * factor + total
            acc[64 * row : 64 * row + 64, :] = acc[64 * row : 64 * row + 64, :] * factor + o

    def score(row, ja, jb, first):
        g, n = row // 4, row % 4
        sa = jnp.dot(kv[ja, 0:128, :], qp[g, n], preferred_element_type=jnp.float32)
        sb = jnp.dot(kv[jb, 0:128, :], qp[g, n], preferred_element_type=jnp.float32)
        if first:
            sa = sa + diag[0:128, :]
            sb = sb + diag[128:256, :]
        s_ref[row, 0:128, :] = sa
        s_ref[row, 128:256, :] = sb
        ma, mb = jnp.max(sa, axis=0, keepdims=True), jnp.max(sb, axis=0, keepdims=True)
        if first:
            new = jnp.maximum(ma, mb)
            mo_ref[0, row : row + 1, :] = new
            mo_ref[1, row : row + 1, :] = new
        else:
            ba = jnp.where(blocks[0:1, :] < order[ja], BIG, 0.0)
            bb = jnp.where(blocks[0:1, :] < order[jb], BIG, 0.0)
            old = m_ref[row : row + 1, :]
            new = jnp.maximum(old, jnp.maximum(ma - ba, mb - bb))
            f_ref[row : row + 1, :] = jnp.exp2(old - new)
            mo_ref[0, row : row + 1, :] = new + ba
            mo_ref[1, row : row + 1, :] = new + bb
        m_ref[row : row + 1, :] = new

    def attend(before, now):
        for row in range(8):
            weigh(row, *before, False)
            score(row, *now, False)
        return now

    for row in range(8):
        score(row, 2 * b, 2 * b + 1, True)
    for row in range(8):
        l_ref[row : row + 1, :] = jnp.zeros((1, 256), jnp.float32)
        acc[64 * row : 64 * row + 64, :] = jnp.zeros((64, 256), jnp.float32)
        f_ref[row : row + 1, :] = jnp.zeros((1, 256), jnp.float32)
    held = (2 * b, 2 * b + 1)

    def source(f, i, ds):
        major, minor = coords[f]
        pp, xx = plane(i, major, x)
        return origin(f, pp, (minor + ds) % 4, xx)

    def take(i, ds):
        for f in range(2):
            major, minor = coords[f]
            org = source(f, i, ds)
            arrived(f, org)
            if ds == 0:
                if i in (1, 2):
                    copy(f, org, origin(f, (major + 1) % 4, minor, x), i, 2).start()
                if i in (1, 5):
                    copy(f, org, origin(f, (major + 3) % 4, minor, x), i, 3).start()
                if i not in (1, 3):
                    copy(f, org, origin(f, major, (minor + 1) % 4, x), i, 0).start()
                    copy(f, org, origin(f, major, (minor + 3) % 4, x), i, 1).start()
            elif ds != 2:
                if i in (0, 2):
                    copy(f, org, origin(f, major, minor, (x + 1) % 2), i + 1, ds // 3).start()
                if (i // 2) % 2 == (ds == 1):
                    copy(f, org, origin(f, major, (minor + 4 - ds) % 4, x), i, 5).start()

    def one_step(n, held):
        for group in range(0, 32, 8):

            @pl.when(n // 8 == group // 8)
            def _():
                for at in range(group, group + 8):
                    if EVENTS[at]:

                        @pl.when(n == at)
                        def _():
                            for i, ds in EVENTS[at]:
                                take(i, ds)

        code = jnp.int32(CODES[-1])
        for part in range(len(CODES) - 2, -1, -1):
            code = jnp.where(n < 6 * part + 6, CODES[part], code)
        code = lax.shift_right_logical(code, 5 * (n % 6)) % 32
        i, ds = code // 4, code % 4
        return attend(held, (2 * source(0, i, ds), 2 * source(1, i, ds) + 1))

    held = lax.fori_loop(0, 31, one_step, held)
    for row in range(8):
        weigh(row, *held, False)

    for n in range(8):
        inv = 1.0 / l_ref[n : n + 1, :]
        heads[:, 64 * n : 64 * n + 64] = (acc[64 * n : 64 * n + 64, :] * inv).T.astype(jnp.bfloat16)

    def sent(i, _):
        for f in range(2):
            for which in (0, 1, 5):
                copy(f, b, peers[0], i, which).wait_send()
        return 0

    lax.fori_loop(0, 8, sent, 0)
    for f in range(2):
        for i, which in ((0, 4), (0, 2), (0, 3), (1, 2), (1, 3), (2, 2), (5, 3)):
            copy(f, b, peers[0], i, which).wait_send()

    def tail_copy(stage, r, src, dst, peer):
        return pltpu.make_async_remote_copy(
            src_ref=src, dst_ref=dst,
            send_sem=tail_send.at[stage, r], recv_sem=tail_recv.at[stage, r],
            device_id={"tp": peer}, device_id_type=MESH,
        )

    def columns(c):
        return pl.ds(pl.multiple_of(c * SHARE, SHARE), SHARE)

    def rows_of(q):
        return slice(PIECE * q, PIECE * q + PIECE)

    def chunk_rows(r):
        return slice(ROWS * r, ROWS * r + ROWS)

    def near_copy(stage, q, j):
        at = rows_of(q)
        return tail_copy(
            (0, 2, 7, 8)[2 * j + stage], q, near_out.at[stage, j, at], near_in.at[stage, j, at], twin
        )

    def far_copy(stage, q):
        return tail_copy(
            2 * stage + 1, q, far_out.at[stage, rows_of(q)], far_in.at[stage, rows_of(q)], across
        )

    def give(stage, pieces, j, lhs, w):
        at = slice(PIECE * pieces[0], PIECE * pieces[-1] + PIECE)
        part = jnp.dot(lhs[at, :], w[:, columns((twin + 2 - 2 * j) % 4)], preferred_element_type=jnp.float32)
        near_out[stage, j, at] = part.astype(jnp.bfloat16)
        for q in pieces:
            near_copy(stage, q, j).start()

    def keep(pieces, j, lhs, w):
        at = slice(PIECE * pieces[0], PIECE * pieces[-1] + PIECE)
        kept[j, at] = jnp.dot(lhs[at, :], w[:, columns((across, t)[j])], preferred_element_type=jnp.float32)

    def cross(stage, q):
        at = rows_of(q)
        near_copy(stage, q, 0).wait()
        far_out[stage, at] = (kept[0, at] + near_in[stage, 0, at].astype(jnp.float32)).astype(jnp.bfloat16)
        far_copy(stage, q).start()

    def total(stage, q):
        at = rows_of(q)
        near_copy(stage, q, 1).wait()
        far_copy(stage, q).wait()
        return kept[1, at] + near_in[stage, 1, at].astype(jnp.float32) + far_in[stage, at].astype(jnp.float32)

    def share_copy(stage, q, slot, peer):
        return tail_copy(stage, q, shares.at[q, slot], shares.at[q, slot], peer)

    def norm_part(q, c, add):
        u = shares[q, c].astype(jnp.float32)
        square = jnp.sum(u * u, axis=-1, keepdims=True)
        squares[rows_of(q), :] = squares[rows_of(q), :] + square if add else jnp.broadcast_to(square, (PIECE, 128))
        normed[rows_of(q), columns(c)] = (u * gain2[:, columns(c)]).astype(jnp.bfloat16)

    every = range(256 // PIECE)
    loads[4].wait()
    give(0, every, 0, heads, wo)
    keep(every, 0, heads, wo)
    give(0, every, 1, heads, wo)
    for q in every:
        cross(0, q)
    keep(every, 1, heads, wo)

    def share_out(q):
        own = tok[rows_of(q), columns(t)].astype(jnp.float32) + total(0, q)
        resid[rows_of(q), :] = own
        shares[q, t] = own.astype(jnp.bfloat16)
        share_copy(4, q, t, across).start()
        share_copy(5, q, t, twin).start()

    def pieces_of(r):
        return range(ROWS // PIECE * r, ROWS // PIECE * (r + 1))

    def pass_on(q):
        share_copy(4, q, across, across).wait_recv()
        share_copy(6, q, across, twin).start()

    def units_pass(r, c, turn):
        for q in pieces_of(r):
            if turn % 2:
                share_copy(5 if turn == 1 else 6, q, c, twin).wait_recv()
            norm_part(q, c, turn > 0)
        if turn == 3:
            scale = lax.rsqrt(squares[chunk_rows(r), 0:1] * (1.0 / (4 * SHARE)) + EPS)

        def units(n, _):
            at = pl.ds(pl.multiple_of(n * UNITS, UNITS), UNITS)
            u = normed[chunk_rows(r), columns(c)]
            gate = jnp.dot(u, wg[columns(c), at], preferred_element_type=jnp.float32)
            up = jnp.dot(u, wu[columns(c), at], preferred_element_type=jnp.float32)
            if turn > 0:
                gate = gate + gated[r, 0, :, at]
                up = up + gated[r, 1, :, at]
            if turn < 3:
                gated[r, 0, :, at] = gate
                gated[r, 1, :, at] = up
            else:
                gate, up = gate * scale, up * scale
                hidden[chunk_rows(r), at] = (gate / (1.0 + jnp.exp(-gate)) * up).astype(jnp.bfloat16)
            return 0

        lax.fori_loop(0, 2048 // UNITS, units, 0)

    def down(r):
        pieces = pieces_of(r)
        give(1, pieces, 0, hidden, wd)
        keep(pieces, 0, hidden, wd)
        give(1, pieces, 1, hidden, wd)
        if r == CHUNKS - 1:
            for q in pieces:
                cross(1, q)
        keep(pieces, 1, hidden, wd)

    share_out(0)
    share_out(1)
    loads[5].wait()
    loads[6].wait()
    units_pass(0, t, 0)
    units_pass(0, twin, 1)
    share_out(2)
    share_out(3)
    units_pass(1, t, 0)
    pass_on(0)
    units_pass(1, twin, 1)
    pass_on(1)
    loads[7].wait()
    units_pass(0, across, 2)
    units_pass(0, (twin + 2) % 4, 3)
    pass_on(2)
    pass_on(3)
    down(0)
    units_pass(1, across, 2)
    cross(1, 0)
    cross(1, 1)
    units_pass(1, (twin + 2) % 4, 3)
    down(1)
    for q in every:
        out[rows_of(q), :] = (resid[rows_of(q), :] + total(1, q)).astype(jnp.bfloat16)
    for q in every:
        share_copy(4, q, t, across).wait_send()
        share_copy(5, q, t, twin).wait_send()
        share_copy(6, q, across, twin).wait_send()


def layer(tok, order, gain, wq, wk, wv, tab, gain2, wo, wg, wu, wd):
    vmem = pl.BlockSpec(memory_space=pltpu.VMEM)
    hbm = pl.BlockSpec(memory_space=pl.ANY)
    bf16, f32 = jnp.bfloat16, jnp.float32
    return pl.pallas_call(
        layer_kernel,
        out_shape=jax.ShapeDtypeStruct((256, SHARE), bf16),
        in_specs=[hbm, pl.BlockSpec(memory_space=pltpu.SMEM), vmem, hbm, hbm, hbm, vmem, vmem, hbm, hbm, hbm, hbm],
        out_specs=vmem,
        scratch_shapes=[
            pltpu.VMEM((256, 256), f32),
            pltpu.VMEM((8, 256), jnp.int32),
            pltpu.VMEM((CHUNKS, 2, ROWS, 2048), f32),
            pltpu.VMEM((256, 128), f32),
            pltpu.VMEM((256, 2048), bf16),
            pltpu.VMEM((2048, 512), bf16),
            pltpu.VMEM((2048, 128), bf16),
            pltpu.VMEM((2048, 128), bf16),
            pltpu.VMEM((512, 2048), bf16),
            pltpu.VMEM((2048, 2048), bf16),
            pltpu.VMEM((2048, 2048), bf16),
            pltpu.VMEM((2048, 2048), bf16),
            pltpu.VMEM((256, 512), bf16),
            pltpu.VMEM((2, 2, 256, SHARE), bf16),
            pltpu.VMEM((2, 2, 256, SHARE), bf16),
            pltpu.VMEM((2, 256, SHARE), bf16),
            pltpu.VMEM((2, 256, SHARE), bf16),
            pltpu.VMEM((2, 256, SHARE), f32),
            pltpu.VMEM((256, SHARE), f32),
            pltpu.VMEM((256 // PIECE, 4, PIECE, SHARE), bf16),
            pltpu.VMEM((256, 2048), bf16),
            pltpu.SemaphoreType.DMA((11,)),
            pltpu.SemaphoreType.DMA((9, 256 // PIECE)),
            pltpu.SemaphoreType.DMA((9, 256 // PIECE)),
            pltpu.VMEM((256, 2048), bf16),
            pltpu.VMEM((64, 256, 128), bf16),
            pltpu.VMEM((2, 4, 128, 256), bf16),
            pltpu.VMEM((8, 256, 256), f32),
            pltpu.VMEM((2, 8, 256), f32),
            pltpu.VMEM((8, 256), f32),
            pltpu.VMEM((8, 256), f32),
            pltpu.VMEM((8, 256), f32),
            pltpu.VMEM((512, 256), f32),
            pltpu.SemaphoreType.DMA((2, 8, 6)),
            pltpu.SemaphoreType.DMA((64,)),
        ],
        compiler_params=pltpu.CompilerParams(
            collective_id=0, has_side_effects=True, vmem_limit_bytes=62 * 1024 * 1024
        ),
        name="layer",
    )(tok, order, gain, wq, wk, wv, tab, gain2, wo, wg, wu, wd)


def local(tokens, order, gain_attn, gain_ffn, w_query, w_key, w_value, w_out, w_gate, w_up, w_down):
    return layer(
        tokens, order, gain_attn[None, :], w_query, w_key, w_value, jnp.asarray(rope_table()),
        gain_ffn[None, :], w_out, w_gate, w_up, w_down,
    )


def solution(mesh):
    placed = (
        P("blk", None),
        P(),
        P(),
        P(),
        P(None, "tp"),
        P(None, "tp"),
        P(None, "tp"),
        P("tp", None),
        P(None, "tp"),
        P(None, "tp"),
        P("tp", None),
    )
    return jax.shard_map(
        local, mesh=mesh, in_specs=placed, out_specs=P("blk", "tp"), check_vma=False
    )
```

```python
import jax
import jax.numpy as jnp
import numpy as np
from jax import lax
from jax.experimental import pallas as pl
from jax.experimental.pallas import tpu as pltpu
from jax.sharding import PartitionSpec as P

HD = 64
SHARE = 512
CHUNKS = 2
ROWS = 256 // CHUNKS
PIECE = 64
UNITS = 512
EPS = 1e-05
ROPE_BASE = 500000.0
BIG = 1e30
LOG2E = 1.4426950408889634
MESH = pl.DeviceIdType.MESH


ORDER = (
    (2, 0), (4, 0), (0, 3), (0, 1), (1, 0), (2, 1), (6, 0), (2, 3),
    (4, 1), (4, 3), (5, 0), (1, 3), (0, 2), (6, 1), (3, 0), (2, 2),
    (1, 1), (6, 3), (7, 0), (5, 3), (5, 1), (3, 1), (4, 2), (6, 2),
    (1, 2), (7, 1), (3, 3), (7, 3), (5, 2), (3, 2), (7, 2),
)
EVENTS = (
    ((2, 0), (4, 0)),
    (),
    ((0, 3), (0, 1)),
    (),
    ((1, 0),),
    ((6, 0), (2, 1)),
    (),
    ((2, 3), (4, 1)),
    (),
    ((5, 0), (4, 3)),
    (),
    ((1, 3),),
    ((0, 2),),
    ((6, 1),),
    ((3, 0),),
    ((2, 2),),
    ((1, 1),),
    ((6, 3), (7, 0)),
    (),
    ((5, 3),),
    ((5, 1),),
    ((3, 1),),
    ((4, 2), (6, 2)),
    (),
    ((1, 2),),
    ((7, 1),),
    ((3, 3), (7, 3)),
    (),
    ((5, 2),),
    ((3, 2),),
    ((7, 2),),
    (),
)
CODES = [sum((4 * i + ds) << (5 * j) for j, (i, ds) in enumerate(ORDER[p : p + 6])) for p in range(0, 31, 6)]


def rope_table():
    freq = ROPE_BASE ** (-np.arange(HD // 2) * 2.0 / HD)[:, None]
    within = freq * np.arange(128)[None, :]
    starts = freq * (128.0 * np.arange(128))[None, :]
    return np.concatenate([np.cos(within), np.sin(within), np.cos(starts), np.sin(starts)]).astype(np.float32)


def origin(flow, major, minor, x):
    if flow == 0:
        return minor * 8 + major * 2 + x
    return major * 8 + minor * 2 + x


def plane(i, major, x):
    k = i // 2
    step = (3 * k + 3 * (k // 2) + 2 * (k // 3)) % 4
    return (major + step) % 4, (x + i) % 2


def layer_kernel(
    tok_hbm, order, gain, wq_hbm, wk_hbm, wv_hbm, tab, gain2, wo_hbm, wg_hbm, wu_hbm, wd_hbm,
    out, diag, blocks, gated, squares, tok, wq, wk, wv, wo, wg, wu, wd, heads, near_out, near_in, far_out, far_in, kept, resid,
    shares, hidden, load_sem, tail_send, tail_recv, normed, kv, qp, s_ref, mo_ref, f_ref, m_ref, l_ref, acc, send_sem, recv_sem,
):
    b = lax.axis_index("blk")
    z, y, x = b // 8, (b // 2) % 4, b % 2
    coords = ((y, z), (z, y))

    t = lax.axis_index("tp")
    core = t % 2
    twin = t + 1 - 2 * core
    across = (t + 2) % 4
    loads = [
        pltpu.make_async_copy(src, dst, load_sem.at[i])
        for i, (src, dst) in enumerate(
            ((tok_hbm.at[0:64], tok.at[0:64]), (wk_hbm, wk), (wv_hbm, wv), (wq_hbm, wq))
            + ((wo_hbm, wo), (wg_hbm, wg), (wu_hbm, wu), (wd_hbm, wd))
        )
    ]
    more = [
        pltpu.make_async_copy(
            tok_hbm.at[64 * r : 64 * r + 64], tok.at[64 * r : 64 * r + 64], load_sem.at[7 + r]
        )
        for r in range(1, 4)
    ]
    for load in (loads[0], *more, *loads[1:4]):
        load.start()
    barrier = pltpu.get_barrier_semaphore()
    for peer in (twin, across):
        pl.semaphore_signal(barrier, inc=1, device_id={"tp": peer}, device_id_type=MESH)
    peers = [origin(0, y, z, (x + 1) % 2)]
    peers += [origin(0, (y + d) % 4, z, x) for d in (1, 3)]
    peers += [origin(0, y, (z + d) % 4, x) for d in (1, 3)]
    for peer in peers:
        pl.semaphore_signal(barrier, inc=1, device_id={"blk": peer}, device_id_type=MESH)

    for r, load in enumerate((loads[0], *more)):
        load.wait()
        at = slice(64 * r, 64 * r + 64)
        wide = tok[at, :].astype(jnp.float32)
        scale = lax.rsqrt(jnp.mean(wide * wide, axis=-1, keepdims=True) + EPS)
        normed[at, :] = (wide * scale * gain[...]).astype(jnp.bfloat16)

    first, second = order[2 * b], order[2 * b + 1]
    lane = lax.broadcasted_iota(jnp.int32, (32, 128), 1)
    cosines, sines = [], []
    for block in (first, second):
        ca = jnp.sum(jnp.where(lane == block, tab[64:96, :], 0.0), axis=1, keepdims=True)
        sa = jnp.sum(jnp.where(lane == block, tab[96:128, :], 0.0), axis=1, keepdims=True)
        cosines.append(ca * tab[0:32, :] - sa * tab[32:64, :])
        sines.append(sa * tab[0:32, :] + ca * tab[32:64, :])
    c = jnp.concatenate(cosines, axis=1)
    s = jnp.concatenate(sines, axis=1)

    def rotated(u):
        a, h = u[0:32], u[32:64]
        return jnp.concatenate([a * c - h * s, h * c + a * s], axis=0)

    loads[1].wait()
    loads[2].wait()
    k = jnp.dot(normed[...], wk[...], preferred_element_type=jnp.float32).T
    kt = jnp.concatenate([rotated(k[0:64]), rotated(k[64:128])], axis=0)
    kn = kt.T.astype(jnp.bfloat16)
    v = jnp.dot(normed[...], wv[...], preferred_element_type=jnp.float32).T.astype(jnp.bfloat16)
    for f in range(2):
        kv[2 * b + f, 0:128, :] = kn[128 * f : 128 * f + 128, :]
        kv[2 * b + f, 128:256, :] = v[:, 128 * f : 128 * f + 128]

    pl.semaphore_wait(barrier, 7)

    def copy(f, org, dest, i, which):
        unit = 2 * org + f
        return pltpu.make_async_remote_copy(
            src_ref=kv.at[unit], dst_ref=kv.at[unit],
            send_sem=send_sem.at[f, i, which], recv_sem=recv_sem.at[unit],
            device_id={"blk": dest}, device_id_type=MESH,
        )

    def arrived(f, org):
        unit = 2 * org + f
        pltpu.make_async_remote_copy(
            src_ref=kv.at[unit], dst_ref=kv.at[unit],
            send_sem=send_sem.at[f, 0, 0], recv_sem=recv_sem.at[unit],
            device_id={"blk": peers[0]}, device_id_type=MESH,
        ).wait_recv()

    for f in range(2):
        major, minor = coords[f]
        copy(f, b, origin(f, major, minor, (x + 1) % 2), 0, 4).start()
    for f in range(2):
        major, minor = coords[f]
        copy(f, b, origin(f, (major + 1) % 4, minor, x), 0, 2).start()
        copy(f, b, origin(f, (major + 3) % 4, minor, x), 0, 3).start()
    for f in range(2):
        major, minor = coords[f]
        copy(f, b, origin(f, major, (minor + 1) % 4, x), 0, 0).start()
        copy(f, b, origin(f, major, (minor + 3) % 4, x), 0, 1).start()

    column = lax.broadcasted_iota(jnp.int32, (8, 256), 1)
    block_row = jnp.where(column < 128, first, second)
    blocks[...] = block_row
    place = block_row[0:1] * 128 + column[0:1] % 128
    for f, block in enumerate((first, second)):
        key_place = block * 128 + lax.broadcasted_iota(jnp.int32, (128, 256), 0)
        diag[128 * f : 128 * f + 128, :] = jnp.where(key_place <= place, 0.0, -BIG)

    loads[3].wait()
    for load in loads[4:]:
        load.start()
    zero = jnp.zeros((64, 256), jnp.bfloat16)
    for half in range(2):
        q = jnp.dot(
            normed[...], wq[:, 256 * half : 256 * half + 256], preferred_element_type=jnp.float32
        ).T
        for n in range(4):
            u = (rotated(q[64 * n : 64 * n + 64]) * (HD**-0.5 * LOG2E)).astype(jnp.bfloat16)
            top, low = (u, zero) if half == 0 else (zero, u)
            qp[half, n, 0:64, :] = top
            qp[half, n, 64:128, :] = low

    def weigh(row, ja, jb, first):
        g, n = row // 4, row % 4
        pa = jnp.exp2(s_ref[row, 0:128, :] - mo_ref[0, row : row + 1, :])
        pb = jnp.exp2(s_ref[row, 128:256, :] - mo_ref[1, row : row + 1, :])
        p = jnp.concatenate([pa, pb], axis=0).astype(jnp.bfloat16)
        va = kv[ja, 128 + 64 * g : 192 + 64 * g, :]
        vb = kv[jb, 128 + 64 * g : 192 + 64 * g, :]
        vt = jnp.concatenate([jnp.concatenate([va, vb], axis=1), jnp.ones((16, 256), jnp.bfloat16)], axis=0)
        o = jnp.dot(vt, p, preferred_element_type=jnp.float32)
        total, o = o[64:65], o[0:64]
        if first:
            l_ref[row : row + 1, :] = total
            acc[64 * row : 64 * row + 64, :] = o
        else:
            factor = f_ref[row : row + 1, :]
            l_ref[row : row + 1, :] = l_ref[row : row + 1, :] * factor + total
            acc[64 * row : 64 * row + 64, :] = acc[64 * row : 64 * row + 64, :] * factor + o

    def score(row, ja, jb, first):
        g, n = row // 4, row % 4
        sa = jnp.dot(kv[ja, 0:128, :], qp[g, n], preferred_element_type=jnp.float32)
        sb = jnp.dot(kv[jb, 0:128, :], qp[g, n], preferred_element_type=jnp.float32)
        if first:
            sa = sa + diag[0:128, :]
            sb = sb + diag[128:256, :]
        s_ref[row, 0:128, :] = sa
        s_ref[row, 128:256, :] = sb
        ma, mb = jnp.max(sa, axis=0, keepdims=True), jnp.max(sb, axis=0, keepdims=True)
        if first:
            new = jnp.maximum(ma, mb)
            mo_ref[0, row : row + 1, :] = new
            mo_ref[1, row : row + 1, :] = new
        else:
            ba = jnp.where(blocks[0:1, :] < order[ja], BIG, 0.0)
            bb = jnp.where(blocks[0:1, :] < order[jb], BIG, 0.0)
            old = m_ref[row : row + 1, :]
            new = jnp.maximum(old, jnp.maximum(ma - ba, mb - bb))
            f_ref[row : row + 1, :] = jnp.exp2(old - new)
            mo_ref[0, row : row + 1, :] = new + ba
            mo_ref[1, row : row + 1, :] = new + bb
        m_ref[row : row + 1, :] = new

    def attend(before, now):
        for row in range(8):
            weigh(row, *before, False)
            score(row, *now, False)
        return now

    for row in range(8):
        score(row, 2 * b, 2 * b + 1, True)
    for row in range(8):
        l_ref[row : row + 1, :] = jnp.zeros((1, 256), jnp.float32)
        acc[64 * row : 64 * row + 64, :] = jnp.zeros((64, 256), jnp.float32)
        f_ref[row : row + 1, :] = jnp.zeros((1, 256), jnp.float32)
    held = (2 * b, 2 * b + 1)

    def source(f, i, ds):
        major, minor = coords[f]
        pp, xx = plane(i, major, x)
        return origin(f, pp, (minor + ds) % 4, xx)

    def take(i, ds):
        for f in range(2):
            major, minor = coords[f]
            org = source(f, i, ds)
            arrived(f, org)
            if ds == 0:
                if i in (1, 2):
                    copy(f, org, origin(f, (major + 1) % 4, minor, x), i, 2).start()
                if i in (1, 5):
                    copy(f, org, origin(f, (major + 3) % 4, minor, x), i, 3).start()
                if i not in (1, 3):
                    copy(f, org, origin(f, major, (minor + 1) % 4, x), i, 0).start()
                    copy(f, org, origin(f, major, (minor + 3) % 4, x), i, 1).start()
            elif ds != 2:
                if i in (0, 2):
                    copy(f, org, origin(f, major, minor, (x + 1) % 2), i + 1, ds // 3).start()
                if (i // 2) % 2 == (ds == 1):
                    copy(f, org, origin(f, major, (minor + 4 - ds) % 4, x), i, 5).start()

    def one_step(n, held):
        for group in range(0, 32, 8):

            @pl.when(n // 8 == group // 8)
            def _():
                for at in range(group, group + 8):
                    if EVENTS[at]:

                        @pl.when(n == at)
                        def _():
                            for i, ds in EVENTS[at]:
                                take(i, ds)

        code = jnp.int32(CODES[-1])
        for part in range(len(CODES) - 2, -1, -1):
            code = jnp.where(n < 6 * part + 6, CODES[part], code)
        code = lax.shift_right_logical(code, 5 * (n % 6)) % 32
        i, ds = code // 4, code % 4
        return attend(held, (2 * source(0, i, ds), 2 * source(1, i, ds) + 1))

    held = lax.fori_loop(0, 31, one_step, held)
    for row in range(8):
        weigh(row, *held, False)

    for n in range(8):
        inv = 1.0 / l_ref[n : n + 1, :]
        heads[:, 64 * n : 64 * n + 64] = (acc[64 * n : 64 * n + 64, :] * inv).T.astype(jnp.bfloat16)

    def sent(i, _):
        for f in range(2):
            for which in (0, 1, 5):
                copy(f, b, peers[0], i, which).wait_send()
        return 0

    lax.fori_loop(0, 8, sent, 0)
    for f in range(2):
        for i, which in ((0, 4), (0, 2), (0, 3), (1, 2), (1, 3), (2, 2), (5, 3)):
            copy(f, b, peers[0], i, which).wait_send()

    def tail_copy(stage, r, src, dst, peer):
        return pltpu.make_async_remote_copy(
            src_ref=src, dst_ref=dst,
            send_sem=tail_send.at[stage, r], recv_sem=tail_recv.at[stage, r],
            device_id={"tp": peer}, device_id_type=MESH,
        )

    def columns(c):
        return pl.ds(pl.multiple_of(c * SHARE, SHARE), SHARE)

    def rows_of(q):
        return slice(PIECE * q, PIECE * q + PIECE)

    def chunk_rows(r):
        return slice(ROWS * r, ROWS * r + ROWS)

    def near_copy(stage, q, j):
        at = rows_of(q)
        return tail_copy(
            (0, 2, 7, 8)[2 * j + stage], q, near_out.at[stage, j, at], near_in.at[stage, j, at], twin
        )

    def far_copy(stage, q):
        return tail_copy(
            2 * stage + 1, q, far_out.at[stage, rows_of(q)], far_in.at[stage, rows_of(q)], across
        )

    def give(stage, pieces, j, lhs, w):
        at = slice(PIECE * pieces[0], PIECE * pieces[-1] + PIECE)
        part = jnp.dot(lhs[at, :], w[:, columns((twin + 2 - 2 * j) % 4)], preferred_element_type=jnp.float32)
        near_out[stage, j, at] = part.astype(jnp.bfloat16)
        for q in pieces:
            near_copy(stage, q, j).start()

    def keep(pieces, j, lhs, w):
        at = slice(PIECE * pieces[0], PIECE * pieces[-1] + PIECE)
        kept[j, at] = jnp.dot(lhs[at, :], w[:, columns((across, t)[j])], preferred_element_type=jnp.float32)

    def cross(stage, q):
        at = rows_of(q)
        near_copy(stage, q, 0).wait()
        far_out[stage, at] = (kept[0, at] + near_in[stage, 0, at].astype(jnp.float32)).astype(jnp.bfloat16)
        far_copy(stage, q).start()

    def total(stage, q):
        at = rows_of(q)
        near_copy(stage, q, 1).wait()
        far_copy(stage, q).wait()
        return kept[1, at] + near_in[stage, 1, at].astype(jnp.float32) + far_in[stage, at].astype(jnp.float32)

    def share_copy(stage, q, slot, peer):
        return tail_copy(stage, q, shares.at[q, slot], shares.at[q, slot], peer)

    def norm_part(q, c, add):
        u = shares[q, c].astype(jnp.float32)
        square = jnp.sum(u * u, axis=-1, keepdims=True)
        squares[rows_of(q), :] = squares[rows_of(q), :] + square if add else jnp.broadcast_to(square, (PIECE, 128))
        normed[rows_of(q), columns(c)] = (u * gain2[:, columns(c)]).astype(jnp.bfloat16)

    every = range(256 // PIECE)
    loads[4].wait()
    give(0, every, 0, heads, wo)
    keep(every, 0, heads, wo)
    give(0, every, 1, heads, wo)
    for q in every:
        cross(0, q)
    keep(every, 1, heads, wo)

    def share_out(q):
        own = tok[rows_of(q), columns(t)].astype(jnp.float32) + total(0, q)
        resid[rows_of(q), :] = own
        shares[q, t] = own.astype(jnp.bfloat16)
        share_copy(4, q, t, across).start()
        share_copy(5, q, t, twin).start()

    def pieces_of(r):
        return range(ROWS // PIECE * r, ROWS // PIECE * (r + 1))

    def pass_on(q):
        share_copy(4, q, across, across).wait_recv()
        share_copy(6, q, across, twin).start()

    def units_pass(r, c, turn):
        for q in pieces_of(r):
            if turn % 2:
                share_copy(5 if turn == 1 else 6, q, c, twin).wait_recv()
            norm_part(q, c, turn > 0)
        if turn == 3:
            scale = lax.rsqrt(squares[chunk_rows(r), 0:1] * (1.0 / (4 * SHARE)) + EPS)

        def units(n, _):
            at = pl.ds(pl.multiple_of(n * UNITS, UNITS), UNITS)
            u = normed[chunk_rows(r), columns(c)]
            gate = jnp.dot(u, wg[columns(c), at], preferred_element_type=jnp.float32)
            up = jnp.dot(u, wu[columns(c), at], preferred_element_type=jnp.float32)
            if turn > 0:
                gate = gate + gated[r, 0, :, at]
                up = up + gated[r, 1, :, at]
            if turn < 3:
                gated[r, 0, :, at] = gate
                gated[r, 1, :, at] = up
            else:
                gate, up = gate * scale, up * scale
                hidden[chunk_rows(r), at] = (gate / (1.0 + jnp.exp(-gate)) * up).astype(jnp.bfloat16)
            return 0

        lax.fori_loop(0, 2048 // UNITS, units, 0)

    def down(r):
        pieces = pieces_of(r)
        give(1, pieces, 0, hidden, wd)
        keep(pieces, 0, hidden, wd)
        give(1, pieces, 1, hidden, wd)
        if r == CHUNKS - 1:
            for q in pieces:
                cross(1, q)
        keep(pieces, 1, hidden, wd)

    share_out(0)
    share_out(1)
    loads[5].wait()
    loads[6].wait()
    units_pass(0, t, 0)
    units_pass(0, twin, 1)
    share_out(2)
    share_out(3)
    units_pass(1, t, 0)
    pass_on(0)
    units_pass(1, twin, 1)
    pass_on(1)
    loads[7].wait()
    units_pass(0, across, 2)
    units_pass(0, (twin + 2) % 4, 3)
    pass_on(2)
    pass_on(3)
    down(0)
    units_pass(1, across, 2)
    cross(1, 0)
    cross(1, 1)
    units_pass(1, (twin + 2) % 4, 3)
    down(1)
    for q in every:
        out[rows_of(q), :] = (resid[rows_of(q), :] + total(1, q)).astype(jnp.bfloat16)
    for q in every:
        share_copy(4, q, t, across).wait_send()
        share_copy(5, q, t, twin).wait_send()
        share_copy(6, q, across, twin).wait_send()


def layer(tok, order, gain, wq, wk, wv, tab, gain2, wo, wg, wu, wd):
    vmem = pl.BlockSpec(memory_space=pltpu.VMEM)
    hbm = pl.BlockSpec(memory_space=pl.ANY)
    bf16, f32 = jnp.bfloat16, jnp.float32
    return pl.pallas_call(
        layer_kernel,
        out_shape=jax.ShapeDtypeStruct((256, SHARE), bf16),
        in_specs=[hbm, pl.BlockSpec(memory_space=pltpu.SMEM), vmem, hbm, hbm, hbm, vmem, vmem, hbm, hbm, hbm, hbm],
        out_specs=vmem,
        scratch_shapes=[
            pltpu.VMEM((256, 256), f32),
            pltpu.VMEM((8, 256), jnp.int32),
            pltpu.VMEM((CHUNKS, 2, ROWS, 2048), f32),
            pltpu.VMEM((256, 128), f32),
            pltpu.VMEM((256, 2048), bf16),
            pltpu.VMEM((2048, 512), bf16),
            pltpu.VMEM((2048, 128), bf16),
            pltpu.VMEM((2048, 128), bf16),
            pltpu.VMEM((512, 2048), bf16),
            pltpu.VMEM((2048, 2048), bf16),
            pltpu.VMEM((2048, 2048), bf16),
            pltpu.VMEM((2048, 2048), bf16),
            pltpu.VMEM((256, 512), bf16),
            pltpu.VMEM((2, 2, 256, SHARE), bf16),
            pltpu.VMEM((2, 2, 256, SHARE), bf16),
            pltpu.VMEM((2, 256, SHARE), bf16),
            pltpu.VMEM((2, 256, SHARE), bf16),
            pltpu.VMEM((2, 256, SHARE), f32),
            pltpu.VMEM((256, SHARE), f32),
            pltpu.VMEM((256 // PIECE, 4, PIECE, SHARE), bf16),
            pltpu.VMEM((256, 2048), bf16),
            pltpu.SemaphoreType.DMA((11,)),
            pltpu.SemaphoreType.DMA((9, 256 // PIECE)),
            pltpu.SemaphoreType.DMA((9, 256 // PIECE)),
            pltpu.VMEM((256, 2048), bf16),
            pltpu.VMEM((64, 256, 128), bf16),
            pltpu.VMEM((2, 4, 128, 256), bf16),
            pltpu.VMEM((8, 256, 256), f32),
            pltpu.VMEM((2, 8, 256), f32),
            pltpu.VMEM((8, 256), f32),
            pltpu.VMEM((8, 256), f32),
            pltpu.VMEM((8, 256), f32),
            pltpu.VMEM((512, 256), f32),
            pltpu.SemaphoreType.DMA((2, 8, 6)),
            pltpu.SemaphoreType.DMA((64,)),
        ],
        compiler_params=pltpu.CompilerParams(
            collective_id=0, has_side_effects=True, vmem_limit_bytes=62 * 1024 * 1024
        ),
        name="layer",
    )(tok, order, gain, wq, wk, wv, tab, gain2, wo, wg, wu, wd)


def local(tokens, order, gain_attn, gain_ffn, w_query, w_key, w_value, w_out, w_gate, w_up, w_down):
    return layer(
        tokens, order, gain_attn[None, :], w_query, w_key, w_value, jnp.asarray(rope_table()),
        gain_ffn[None, :], w_out, w_gate, w_up, w_down,
    )


def solution(mesh):
    placed = (
        P("blk", None),
        P(),
        P(),
        P(),
        P(None, "tp"),
        P(None, "tp"),
        P(None, "tp"),
        P("tp", None),
        P(None, "tp"),
        P(None, "tp"),
        P("tp", None),
    )
    return jax.shard_map(
        local, mesh=mesh, in_specs=placed, out_specs=P("blk", "tp"), check_vma=False
    )
```
